256 devices in a mesh: seq: 64 (over z, y, core), head: 4 (over x).
Axes of the slice: x: 4, y: 4, z: 8, core: 2. Of those that a mesh axis runs over, the one named last changes fastest.
Arguments:
- queries: bfloat16 [32768, 8192], P(('seq', 'head')), may hold values from -8 to 8
- keys: bfloat16 [32768, 1024], P(('seq', 'head')), may hold values from -8 to 8
- values: bfloat16 [32768, 1024], P(('seq', 'head')), may hold values from -6 to 6
- selected: int32 [256, 8], P('seq'), may hold values from 0 to 255, as said below
- counts: int32 [256], P('seq'), may hold values from 1 to 8
- block_slot: int32 [256], P('seq'), may hold values from 0 to 255, as said below
Outputs:
- attended: bfloat16 [32768, 8192], P(('seq', 'head'))
The draws below stay inside these ranges and needn't reach their ends.
Inputs may be any that keep to these rules, and one draw needn't show every extreme that they name: A permutation of 0 to 255. Block b's rows of keys and values start at row 128 * block_slot[b]; its owner shard is block_slot[b] // 4. The 4 blocks of one sequence shard (blocks s * 4 onward) have distinct owner shards, and block_slot[b] % 4 == b % 4. `selected`: row q lists its live entries first: entry 0 is q itself, the other live entries are distinct blocks of earlier sequence shards; entries from counts[q] on are 0. Over the live entries of the 4 rows of one sequence shard, at most 2 distinct blocks have the same owner shard, and in every draw some shard reaches 2 from some owner.
All inputs are finite; a program needn't handle non-finite values.
Results may differ from the reference program's by a relative error of at most 0.0049.
Values may be sent and summed in bfloat16 or wider, within the bound.
A program may use at most 128 MiB of HBM per device.

```python
import math
import jax
import jax.numpy as jnp
from jax import lax

QUERY_HEADS = 64
KEY_VALUE_HEADS = 8
HEAD_SIZE = 128
BLOCK_ROWS = 128
SELECTION_COUNT = 8
BLK_SEQ = 4
NB = 256
TOKEN_COUNT = 32768
N_SEQ = 64


def selection_tables(key):
    base = jax.random.fold_in(key, 4049)
    keys_list = jax.random.split(base, 5)
    shard_perm = jax.random.permutation(keys_list[0], N_SEQ).astype(jnp.int32)
    offsets = jax.random.permutation(keys_list[1], N_SEQ)[:BLK_SEQ].astype(jnp.int32)
    blocks = jnp.arange(NB, dtype=jnp.int32)
    home_shard = blocks // BLK_SEQ
    within = blocks % BLK_SEQ
    owner_of = (shard_perm[home_shard] + offsets[within]) % N_SEQ
    slot_of = owner_of * BLK_SEQ + within
    by_slot = jnp.zeros((NB,), jnp.int32).at[slot_of].set(blocks)
    slot_grid = by_slot.reshape(N_SEQ, BLK_SEQ)
    grid_shard = slot_grid // BLK_SEQ
    rank_draw = jax.random.randint(keys_list[2], (N_SEQ, N_SEQ, BLK_SEQ), 0, 1 << 20) * BLK_SEQ + jnp.arange(BLK_SEQ, dtype=jnp.int32)
    requesters = jnp.arange(N_SEQ, dtype=jnp.int32)[:, None, None]
    masked = jnp.where(grid_shard[None] < requesters, rank_draw, -1)
    best_pick = jnp.argmax(masked, axis=2).astype(jnp.int32)
    extra_ok = jnp.max(masked, axis=2) >= 0
    spread_grid = jnp.broadcast_to(slot_grid[None], (N_SEQ, N_SEQ, BLK_SEQ))
    extra_block = jnp.take_along_axis(spread_grid, best_pick[:, :, None], axis=2)[:, :, 0]
    priority = jax.random.randint(keys_list[3], (NB, N_SEQ), 0, 1 << 20) * N_SEQ + jnp.arange(N_SEQ, dtype=jnp.int32)[None, :]
    first_owner = owner_of[home_shard * BLK_SEQ]
    forced = (within == BLK_SEQ - 1)[:, None] & (jnp.arange(N_SEQ, dtype=jnp.int32)[None, :] == first_owner[:, None])
    priority = jnp.where(forced, 1 << 30, priority)
    usable = extra_ok[home_shard]
    priority = jnp.where(usable, priority, -1)
    top_values, top_index = lax.top_k(priority, SELECTION_COUNT - 1)
    picked = jnp.take_along_axis(extra_block[home_shard], top_index, axis=1)
    pool_size = jnp.sum(usable.astype(jnp.int32), axis=1)
    want_count = jax.random.randint(keys_list[4], (NB,), SELECTION_COUNT // 2, SELECTION_COUNT)
    extra_count = jnp.minimum(want_count, pool_size).astype(jnp.int32)
    position = jnp.arange(SELECTION_COUNT - 1, dtype=jnp.int32)[None, :]
    picked = jnp.where(position < extra_count[:, None], picked, 0).astype(jnp.int32)
    chosen = jnp.concatenate([blocks[:, None], picked], axis=1).astype(jnp.int32)
    return (slot_of.astype(jnp.int32), chosen, (1 + extra_count).astype(jnp.int32))


def draw_selected(key, part):
    return selection_tables(key)[1]


def draw_counts(key, part):
    return selection_tables(key)[2]


def draw_block_slot(key, part):
    return selection_tables(key)[0]


def draw_queries(key, part):
    random_portion = jax.random.normal(jax.random.fold_in(key, 11), (TOKEN_COUNT, QUERY_HEADS, HEAD_SIZE), jnp.float32)
    sampled_blocks = random_portion
    return jnp.clip(sampled_blocks, -8.0, 8.0).reshape(TOKEN_COUNT, QUERY_HEADS * HEAD_SIZE).astype(jnp.bfloat16)


def draw_keys(key, part):
    random_portion = jax.random.normal(jax.random.fold_in(key, 21), (TOKEN_COUNT, KEY_VALUE_HEADS, HEAD_SIZE), jnp.float32)
    sampled_blocks = random_portion
    return jnp.clip(sampled_blocks, -8.0, 8.0).reshape(TOKEN_COUNT, KEY_VALUE_HEADS * HEAD_SIZE).astype(jnp.bfloat16)


def shard_levels(stream_key, dims, pieces, least, largest):
    def one(dim, shards_of):
        heights = jax.random.uniform(jax.random.fold_in(jax.random.fold_in(stream_key, 6), dim), (shards_of,), jnp.float32, least / len(pieces), largest / len(pieces))
        return jnp.repeat(jnp.exp(heights), dims[dim] // shards_of).reshape((-1,) + (1,) * (len(dims) - dim - 1))

    level = one(*pieces[0])
    for cut in pieces[1:]:
        level = level * one(*cut)
    return level


def centred(key, dims, width, limit, cuts=(), kind=jnp.bfloat16):
    gain = shard_levels(key, dims, cuts, -0.22, 0.18) if cuts else 1.0
    entries = jax.random.normal(key, dims, jnp.float32) * width * gain
    return jnp.minimum(jnp.maximum(entries, -limit), limit).astype(kind)


def setup_inputs(seed: int = 0) -> dict:
    splits = jax.random.split(jax.random.key(seed), 7)
    queries = draw_queries(jax.random.fold_in(splits[6], 71), 0)
    keys = draw_keys(jax.random.fold_in(splits[6], 71), 0)
    values = centred(splits[2], (TOKEN_COUNT, KEY_VALUE_HEADS * HEAD_SIZE), 1.0, 6.0, ((0, 256),))
    selected = draw_selected(jax.random.fold_in(splits[6], 71), 0)
    counts = draw_counts(jax.random.fold_in(splits[6], 71), 0)
    block_slot = draw_block_slot(jax.random.fold_in(splits[6], 71), 0)
    return dict(queries=queries, keys=keys, values=values, selected=selected, counts=counts, block_slot=block_slot)


def reference(queries, keys, values, selected, counts, block_slot):
    block_count = selected.shape[0]
    heads_per_group = QUERY_HEADS // KEY_VALUE_HEADS
    score_scale = 1.0 / math.sqrt(HEAD_SIZE)
    key_block_list = keys.reshape(block_count, BLOCK_ROWS, KEY_VALUE_HEADS, HEAD_SIZE)
    value_block_list = values.reshape(block_count, BLOCK_ROWS, KEY_VALUE_HEADS, HEAD_SIZE)
    query_block_list = queries.reshape(block_count, BLOCK_ROWS, KEY_VALUE_HEADS, heads_per_group, HEAD_SIZE)

    def one_block(operands):
        block_id, query_tile, chosen, live_count = operands
        holder_shard = block_slot[chosen]
        key_block_rows = key_block_list[holder_shard].reshape(SELECTION_COUNT * BLOCK_ROWS, KEY_VALUE_HEADS, HEAD_SIZE)
        value_block_rows = value_block_list[holder_shard].reshape(SELECTION_COUNT * BLOCK_ROWS, KEY_VALUE_HEADS, HEAD_SIZE)
        scores = jnp.einsum('igmd,kgd->gmik', query_tile.astype(jnp.float32), key_block_rows.astype(jnp.float32)) * score_scale
        query_pos = block_id * BLOCK_ROWS + jnp.arange(BLOCK_ROWS, dtype=jnp.int32)
        key_pos = (chosen[:, None] * BLOCK_ROWS + jnp.arange(BLOCK_ROWS, dtype=jnp.int32)[None, :]).reshape(-1)
        live_entry = jnp.repeat(jnp.arange(SELECTION_COUNT, dtype=jnp.int32) < live_count, BLOCK_ROWS)
        visible = live_entry[None, :] & (key_pos[None, :] <= query_pos[:, None])
        scores = jnp.where(visible[None, None], scores, -jnp.inf)
        row_top = lax.optimization_barrier(jnp.max(scores, axis=-1, keepdims=True))
        weights = jnp.exp(scores - row_top)
        probability = (weights / lax.optimization_barrier(jnp.sum(weights, axis=-1, keepdims=True))).astype(jnp.bfloat16)
        mixed_out = jnp.einsum('gmik,kgd->igmd', probability.astype(jnp.float32), value_block_rows.astype(jnp.float32))
        return mixed_out.astype(jnp.bfloat16).reshape(BLOCK_ROWS, QUERY_HEADS * HEAD_SIZE)
    attended = lax.map(one_block, (jnp.arange(block_count, dtype=jnp.int32), query_block_list, selected, counts))
    return attended.reshape(block_count * BLOCK_ROWS, QUERY_HEADS * HEAD_SIZE)
```

```python
import functools
import math

import jax
import jax.numpy as jnp
from jax import lax
from jax.experimental import pallas as pl
from jax.experimental.pallas import tpu as pltpu
from jax.sharding import PartitionSpec as P

MESH = pl.DeviceIdType.MESH
ROWS = 128
D = 128
NX, NY, NZ = 4, 4, 8
GROUP = 8
SEL = 8
HELD = NZ * GROUP
GQ = 8
FAST = 22
SCALE2 = math.log2(math.e) / math.sqrt(D)


def kernel(U, place_ref, live_ref, list_ref, q_ref, k_ref, v_ref, out_ref,
           qbuf, kz, vz, ku, vu, pack, krl, vrl, cat, pbuf, obuf,
           ex_send, ex_recv, z_send, z_recv, b_send, b_recv, o_send, o_recv, loc):
    H = U // 2
    s = lax.axis_index("seq")
    x = lax.axis_index("head")
    c = s % 2
    y = (s // 2) % NY
    z = s // (2 * NY)
    a = x * (1 - c) + y * c
    b = y * (1 - c) + x * c
    g = a + 4 * c
    me = 2 * a + c

    def dev(xx, yy, zz, cc):
        return ((zz * NY + yy) * 2 + cc, xx)

    def dev_ab(aa, bb, zz, cc):
        return dev(aa * (1 - c) + bb * c, bb * (1 - c) + aa * c, zz, cc)

    def remote(src, dst, send, recv, target):
        return pltpu.make_async_remote_copy(src_ref=src, dst_ref=dst, send_sem=send, recv_sem=recv,
                                            device_id=target, device_id_type=MESH)

    barrier = pltpu.get_barrier_semaphore()

    def greet(target):
        pl.semaphore_signal(barrier, inc=1, device_id=target, device_id_type=MESH)

    greet(dev(x, y, z, 1 - c))
    for i in range(1, 4):
        for cc in range(2):
            greet(dev((x + i) % NX, y, z, cc))
            greet(dev(x, (y + i) % NY, z, cc))
    greet(dev(x, y, (z + 1) % NZ, c))
    greet(dev(x, y, (z + 7) % NZ, c))
    pl.semaphore_wait(barrier, 15)

    kinds = ((k_ref, kz, D), (v_ref, vz, D), (q_ref, qbuf, GQ * D))

    def piece(kind, t, i):
        src, dst, width = kinds[kind]
        other = (x + i) % NX if t == 0 else (y + i) % NY
        head = other + 4 * t
        slot = (2 * x + c) if t == 0 else (2 * y + c)
        at = slot if kind == 2 else z * GROUP + slot
        target = dev(other, y, z, 0) if t == 0 else dev(x, other, z, 1)
        src = src.at[:, pl.ds(pl.multiple_of(head * width, width), width)]
        return src, dst.at[at], kind, t * 4 + i, slot, target

    def send_piece(kind, t, i):
        src, dst, kind, n, slot, target = piece(kind, t, i)
        remote(src, dst, ex_send.at[kind, n], ex_recv.at[kind, slot], target).start()

    def each_piece(kind, go_remote, go_local):
        for i in (2, 1, 3):
            for t in range(2):
                go_remote(kind, t, i)
        for t in range(2):
            @pl.when(c == t)
            def _():
                go_local(kind, t)

            @pl.when(c != t)
            def _():
                go_remote(kind, t, 0)

    def local_piece(kind, t):
        src, dst, _, _, _, _ = piece(kind, t, 0)
        return pltpu.make_async_copy(src, dst, loc.at[kind])

    for kind in range(3):
        each_piece(kind, send_piece, lambda kind, t: local_piece(kind, t).start())

    def wait_exchange(kind):
        _, dst, _ = kinds[kind]

        def one(i, cc):
            aa = (a + i) % 4
            slot = 2 * aa + cc
            at = slot if kind == 2 else z * GROUP + slot
            remote(dst.at[at], dst.at[at], ex_send.at[kind, 0], ex_recv.at[kind, slot], dev_ab(aa, b, z, cc)).wait_recv()

        for i in range(1, 4):
            for cc in range(2):
                one(i, cc)
        one(0, 1 - c)
        for t in range(2):
            @pl.when(c == t)
            def _():
                local_piece(kind, t).wait()

    def z_copy(kind, way, step, receive):
        buf = (kz, vz)[kind]
        hop = step if receive else step - 1
        chunk = (z - hop + NZ) % NZ if way == 0 else (z + hop) % NZ
        first, count = (0, GROUP) if step < 4 else ((0, GROUP // 2) if way == 0 else (GROUP // 2, GROUP // 2))
        part = buf.at[pl.ds(chunk * GROUP + first, count)]
        target = dev(x, y, (z + 1) % NZ if way == 0 else (z + 7) % NZ, c)
        return remote(part, part, z_send.at[kind, way, step - 1], z_recv.at[kind, way, step - 1], target)

    def z_start(kind, step):
        for way in range(2):
            z_copy(kind, way, step, False).start()

    def z_wait(kind, step):
        for way in range(2):
            z_copy(kind, way, step, True).wait_recv()

    up = dev_ab(a, (b + 1) % 4, z, c)
    down = dev_ab(a, (b + 3) % 4, z, c)

    def b_copy(kind, n):
        have = (ku, vu)[kind]
        rel = (krl, vrl)[kind]
        src, dst, target = (
            (pack.at[pl.ds(0, U)], have.at[pl.ds(HELD, U)], up),
            (pack.at[pl.ds(2 * U, U)], have.at[pl.ds(HELD + 2 * U, U)], down),
            (pack.at[pl.ds(U, H)], rel.at[pl.ds(0, H)], up),
            (pack.at[pl.ds(U + H, H)], rel.at[pl.ds(H, H)], down),
            (rel.at[pl.ds(0, H)], have.at[pl.ds(HELD + U, H)], up),
            (rel.at[pl.ds(H, H)], have.at[pl.ds(HELD + U + H, H)], down),
        )[n]
        return remote(src, dst, b_send.at[kind, n], b_recv.at[kind, n], target)

    def b_begin(kind):
        held = (kz, vz)[kind]
        have = (ku, vu)[kind]
        keep = pltpu.make_async_copy(held, have.at[pl.ds(0, HELD)], loc.at[3 + kind])
        keep.start()

        def one(r, _):
            pack[r] = held[list_ref[r]]
            return 0

        lax.fori_loop(0, 3 * U, one, 0)
        for n in (2, 3, 0, 1):
            b_copy(kind, n).start()

    def b_relay(kind):
        for n in (2, 3):
            b_copy(kind, n).wait_recv()
            b_copy(kind, n + 2).start()

    def b_end(kind):
        for n in (0, 1, 4, 5):
            b_copy(kind, n).wait_recv()
        held = (kz, vz)[kind]
        have = (ku, vu)[kind]
        pltpu.make_async_copy(held, have.at[pl.ds(0, HELD)], loc.at[3 + kind]).wait()

    def b_sent(kind):
        for n in range(6):
            b_copy(kind, n).wait_send()

    row = lax.broadcasted_iota(jnp.int32, (2 * ROWS, ROWS), 0) % ROWS
    col = lax.broadcasted_iota(jnp.int32, (2 * ROWS, ROWS), 1)
    seen = col <= row

    def scores(m, _):
        for e in range(SEL):
            cat[e * ROWS : (e + 1) * ROWS, :] = ku[place_ref[m * SEL + e]]
        live = live_ref[m]
        bias = [jnp.where(e < live, 0.0, -jnp.inf).astype(jnp.float32) for e in range(SEL)]

        def heads(h, _):
            two = qbuf[m, :, pl.ds(pl.multiple_of(h * 2 * D, 2 * D), 2 * D)]
            two = jnp.concatenate([two[:, :D], two[:, D:]], axis=0)
            sc = lax.dot_general(two, cat[...], (((1,), (1,)), ((), ())), preferred_element_type=jnp.float32)
            parts = [jnp.where(seen, sc[:, :ROWS], -jnp.inf)]
            parts += [sc[:, e * ROWS : (e + 1) * ROWS] + bias[e] for e in range(1, SEL)]
            top = functools.reduce(jnp.maximum, parts)
            top = jnp.max(top, axis=1, keepdims=True)
            parts = [jnp.exp2((p - top) * SCALE2) for p in parts]
            total = jnp.sum(functools.reduce(jnp.add, parts), axis=1, keepdims=True)
            inv = 1.0 / total
            at = pl.ds(pl.multiple_of(h * 2 * ROWS, 2 * ROWS), 2 * ROWS)
            for e in range(SEL):
                pbuf[m, at, e * ROWS : (e + 1) * ROWS] = (parts[e] * inv).astype(jnp.bfloat16)
            return 0

        lax.fori_loop(0, GQ // 2, heads, 0)
        return 0

    def out_copy(t):
        i, cc = t // 2, t % 2
        aa = (a + i) % 4
        m = 2 * aa + cc
        src = obuf.at[m]
        dst = out_ref.at[:, pl.ds(pl.multiple_of(g * GQ * D, GQ * D), GQ * D)]
        return m, src, dst, remote(src, dst, o_send.at[t], o_recv.at[g], dev_ab(aa, b, z, cc))

    def attend(n, _):
        t = 7 - n
        m, src, dst, far = out_copy(t)
        for e in range(SEL):
            cat[e * ROWS : (e + 1) * ROWS, :] = vu[place_ref[m * SEL + e]]

        def heads(h, _):
            at = pl.ds(pl.multiple_of(h * 2 * ROWS, 2 * ROWS), 2 * ROWS)
            o = jnp.dot(pbuf[m, at, :], cat[...], preferred_element_type=jnp.float32).astype(jnp.bfloat16)
            first = pl.multiple_of(h * 2 * D, 2 * D)
            obuf[m, :, pl.ds(first, D)] = o[:ROWS]
            obuf[m, :, pl.ds(pl.multiple_of(first + D, D), D)] = o[ROWS:]
            return 0

        lax.fori_loop(0, GQ // 2, heads, 0)

        @pl.when(t == c)
        def _():
            pltpu.make_async_copy(src, dst, loc.at[5]).start()

        @pl.when(t != c)
        def _():
            far.start()

        return 0

    wait_exchange(0)
    z_start(0, 1)
    for step in range(1, 4):
        z_wait(0, step)
        z_start(0, step + 1)
    wait_exchange(1)
    z_wait(0, 4)
    z_start(1, 1)
    b_begin(0)
    b_relay(0)
    for step in range(1, 4):
        z_wait(1, step)
        z_start(1, step + 1)
    wait_exchange(2)
    b_end(0)
    b_sent(0)
    lax.fori_loop(0, 2, scores, 0)
    z_wait(1, 4)
    b_begin(1)
    lax.fori_loop(2, 4, scores, 0)
    b_relay(1)
    lax.fori_loop(4, 8, scores, 0)
    b_end(1)
    lax.fori_loop(0, 8, attend, 0)

    for kind in range(3):
        def sent(kind, t, i):
            src, dst, kind, n, slot, target = piece(kind, t, i)
            remote(src, dst, ex_send.at[kind, n], ex_recv.at[kind, slot], target).wait_send()

        each_piece(kind, sent, lambda kind, t: None)
    for kind in range(2):
        for step in range(1, 5):
            for way in range(2):
                z_copy(kind, way, step, False).wait_send()
    b_sent(1)
    for t in range(8):
        m, src, dst, far = out_copy(t)

        if t < 2:
            @pl.when(c != t)
            def _():
                far.wait_send()

            @pl.when(c == t)
            def _():
                pltpu.make_async_copy(src, dst, loc.at[5]).wait()
        else:
            far.wait_send()
    for h in range(8):
        dst = out_ref.at[:, pl.ds(h * GQ * D, GQ * D)]
        source = dev(h % 4, y, z, 0) if h < 4 else dev(x, h % 4, z, 1)

        @pl.when(g != h)
        def _():
            remote(dst, dst, o_send.at[0], o_recv.at[h], source).wait_recv()


def attention(U, ident, place, live, lists, queries, keys, values):
    any_space = pl.BlockSpec(memory_space=pl.ANY)
    smem = pl.BlockSpec(memory_space=pltpu.SMEM)
    block = (ROWS, D)
    bf16 = jnp.bfloat16
    dma = pltpu.SemaphoreType.DMA
    return pl.pallas_call(
        functools.partial(kernel, U),
        out_shape=jax.ShapeDtypeStruct(queries.shape, bf16),
        in_specs=[smem] * 3 + [any_space] * 3,
        out_specs=any_space,
        scratch_shapes=[
            pltpu.VMEM((GROUP, ROWS, GQ * D), bf16),
            pltpu.VMEM((HELD, *block), bf16),
            pltpu.VMEM((HELD, *block), bf16),
            pltpu.VMEM((HELD + 3 * U, *block), bf16),
            pltpu.VMEM((HELD + 3 * U, *block), bf16),
            pltpu.VMEM((3 * U, *block), bf16),
            pltpu.VMEM((U, *block), bf16),
            pltpu.VMEM((U, *block), bf16),
            pltpu.VMEM((SEL * ROWS, D), bf16),
            pltpu.VMEM((GROUP, GQ * ROWS, SEL * ROWS), bf16),
            pltpu.VMEM((GROUP, ROWS, GQ * D), bf16),
            dma((3, 8)), dma((3, 8)),
            dma((2, 2, 4)), dma((2, 2, 4)),
            dma((2, 6)), dma((2, 6)),
            dma((8,)), dma((8,)),
            dma((6,)),
        ],
        compiler_params=pltpu.CompilerParams(
            collective_id=ident, has_side_effects=True, vmem_limit_bytes=61 * 1024 * 1024),
    )(place, live, lists, queries, keys, values)


def body(queries, keys, values, selected, counts, block_slot):
    s = lax.axis_index("seq")
    x = lax.axis_index("head")
    c = s % 2
    y = (s // 2) % NY
    z = s // (2 * NY)
    b = jnp.where(c == 0, y, x)
    table = jnp.concatenate([selected, counts[:, None], block_slot[:, None]], axis=1)
    table = lax.all_gather(table, "seq", axis=0, tiled=True)
    sel, count, slots = table[:, :SEL], table[:, SEL], table[:, SEL + 1]
    nb = sel.shape[0]
    ids = jnp.arange(nb, dtype=jnp.int32)
    hit = (sel.reshape(-1)[:, None] == ids[None, :]).astype(jnp.bfloat16)
    slot = jnp.dot(hit, slots.astype(jnp.bfloat16)[:, None], preferred_element_type=jnp.float32)
    slot = slot.astype(jnp.int32).reshape(nb, SEL)
    slot = jnp.where(jnp.arange(SEL, dtype=jnp.int32)[None, :] < count[:, None], slot, -1)

    want = jnp.any(slot[:, :, None] == ids[None, None, :], axis=1)
    want = want.reshape(NZ, NY, 2, NX, nb)
    same_y = jnp.any(want, axis=(2, 3)).reshape(NZ * NY, NZ, NY, 2 * NX)
    same_x = jnp.any(want, axis=(1, 2)).reshape(NZ * NX, NZ * NY * 2, NX)
    n_y = jnp.sum(same_y.astype(jnp.int32), axis=(1, 3)).reshape(NZ, NY, NY)
    n_x = jnp.sum(same_x.astype(jnp.int32), axis=1).reshape(NZ, NX, NX)
    apart = jnp.arange(NY)[:, None] != jnp.arange(NY)[None, :]
    most = jnp.max(jnp.where(apart[None], jnp.maximum(n_y, n_x), 0))

    mine = lax.dynamic_slice_in_dim(slot.reshape(NZ, NY, 2, NX, SEL), z, 1, 0)[0]
    live = lax.dynamic_slice_in_dim(count.reshape(NZ, NY, 2, NX), z, 1, 0)[0]

    def arrange(t):
        rest = t.shape[3:]
        along_x = jnp.swapaxes(t, 1, 2).reshape(NY, GROUP, *rest)
        along_y = jnp.moveaxis(t, 2, 0).reshape(NX, GROUP, *rest)
        return jnp.where(c == 0, along_x, along_y)

    groups = arrange(mine).reshape(4, GROUP * SEL)
    sx, so = groups % NX, groups // NX
    sc, sy, sz = so % 2, (so // 2) % NY, so // (2 * NY)
    sa, sb = jnp.where(c == 0, sx, sy), jnp.where(c == 0, sy, sx)
    local = sz * GROUP + 2 * sa + sc
    sb = jnp.where(groups < 0, -1, sb)
    held = jnp.arange(HELD, dtype=jnp.int32)
    order = jnp.arange(4, dtype=jnp.int32)
    hits = (local[:, None, :, None] == held) & (sb[:, None, :, None] == order[None, :, None, None])
    wanted = jnp.any(hits, axis=2).astype(jnp.int32)
    earlier = (held[:, None] < held[None, :]).astype(jnp.int32)
    rank = jnp.sum(wanted[..., :, None] * earlier, axis=2)
    own = lax.dynamic_index_in_dim(rank, b, 0, False)
    out_rank = lax.dynamic_index_in_dim(rank, b, 1, False)
    out_want = lax.dynamic_index_in_dim(wanted, b, 1, False)
    entry_l = lax.dynamic_index_in_dim(local, b, 0, False)
    entry_b = lax.dynamic_index_in_dim(sb, b, 0, False)
    pick = ((entry_l[:, None] == held)[:, None, :] & (entry_b[:, None] == order)[:, :, None])
    entry_rank = jnp.sum(jnp.where(pick, own[None], 0), axis=(1, 2))
    gap = (b - entry_b + 4) % 4

    def place_of(U):
        far = HELD + (gap - 1) * U + entry_rank
        at = jnp.where(entry_b == b, entry_l, far)
        return jnp.where(entry_b < 0, 0, jnp.clip(at, 0, HELD + 3 * U - 1))

    live_mine = lax.dynamic_index_in_dim(arrange(live), b, 0, False)

    def list_of(U):
        r = jnp.arange(U, dtype=jnp.int32)
        chosen = (out_want[:, None, :] > 0) & (out_rank[:, None, :] == r[None, :, None])
        full = jnp.sum(jnp.where(chosen, held[None, None, :], 0), axis=2)
        turned = [lax.dynamic_index_in_dim(full, (b + j) % 4, 0, False) for j in (1, 2, 3)]
        return jnp.concatenate(turned)

    def run(U, ident):
        return lambda: attention(U, ident, place_of(U), live_mine, list_of(U), queries, keys, values)

    return lax.cond(most <= FAST, run(FAST, 0), run(HELD, 1))


def solution(mesh):
    return jax.shard_map(
        body,
        mesh=mesh,
        in_specs=(
            P(("seq", "head"), None),
            P(("seq", "head"), None),
            P(("seq", "head"), None),
            P("seq", None),
            P("seq"),
            P("seq"),
        ),
        out_specs=P(("seq", "head"), None),
        check_vma=False,
    )
```

```python
import functools
import math

import jax
import jax.numpy as jnp
from jax import lax
from jax.experimental import pallas as pl
from jax.experimental.pallas import tpu as pltpu
from jax.sharding import PartitionSpec as P

MESH = pl.DeviceIdType.MESH
ROWS = 128
D = 128
NX, NY, NZ = 4, 4, 8
GROUP = 8
SEL = 8
HELD = NZ * GROUP
GQ = 8
FAST = (16, 12)
NEAR, AFAR = 5 * GROUP, 3 * GROUP
FULL = (NEAR, AFAR)
TW = 64
SCALE2 = math.log2(math.e) / math.sqrt(D)


def kernel(U, key_ref, slot_ref, q_ref, k_ref, v_ref, out_ref, flag_ref,
           qbuf, kn, kf, vn, vf, ku, vu, pack, krl, vrl, cat, pbuf, obuf, orl, keyt, slott, wants, index, smem, flags,
           ex_send, ex_recv, z_send, z_recv, b_send, b_recv, o_send, o_recv, r_recv, t_send, t_recv, loc):
    s = lax.axis_index("seq")
    x = lax.axis_index("head")
    c = s % 2
    y = (s // 2) % NY
    z = s // (2 * NY)
    a = x * (1 - c) + y * c
    b = y * (1 - c) + x * c
    g = a + 4 * c
    r0 = y * 2 + c

    def dev(xx, yy, zz, cc):
        return ((zz * NY + yy) * 2 + cc, xx)

    def dev_ab(aa, bb, zz, cc):
        return dev(aa * (1 - c) + bb * c, bb * (1 - c) + aa * c, zz, cc)

    def remote(src, dst, send, recv, target):
        return pltpu.make_async_remote_copy(src_ref=src, dst_ref=dst, send_sem=send, recv_sem=recv,
                                            device_id=target, device_id_type=MESH)

    barrier = pltpu.get_barrier_semaphore()

    def greet(target):
        pl.semaphore_signal(barrier, inc=1, device_id=target, device_id_type=MESH)

    greet(dev(x, y, z, 1 - c))
    for i in range(1, 4):
        for cc in range(2):
            greet(dev((x + i) % NX, y, z, cc))
            greet(dev(x, (y + i) % NY, z, cc))
    for i in range(1, NZ):
        greet(dev(x, y, (z + i) % NZ, c))
    pl.semaphore_wait(barrier, 20)

    def t_copy(n, receive):
        other = (r0 + n) % 8
        row = other if receive else r0
        target = dev(x, other // 2, z, other % 2)
        sem = (8 - n) % 8 if receive else n
        return (
            remote(key_ref, keyt.at[row], t_send.at[0, n], t_recv.at[0, sem], target),
            remote(slot_ref, slott.at[z, pl.ds(row, 1)], t_send.at[1, n], t_recv.at[1, sem], target),
        )

    def tz_copy(kind, n, receive):
        other = (z + n) % NZ
        row = other if receive else z
        sem = (8 - n) % 8 if receive else n
        buf = (slott, flags)[kind]
        return remote(buf.at[row], buf.at[row], t_send.at[2 + kind, n], t_recv.at[2 + kind, sem], dev(x, y, other, c))

    def t_local():
        return (pltpu.make_async_copy(key_ref, keyt.at[r0], loc.at[6]),
                pltpu.make_async_copy(slot_ref, slott.at[z, pl.ds(r0, 1)], loc.at[7]))

    kinds = ((k_ref, kn, D), (v_ref, vn, D), (q_ref, qbuf, GQ * D))

    def piece(kind, t, i):
        src, dst, width = kinds[kind]
        other = (x + i) % NX if t == 0 else (y + i) % NY
        head = other + 4 * t
        slot = (2 * x + c) if t == 0 else (2 * y + c)
        target = dev(other, y, z, 0) if t == 0 else dev(x, other, z, 1)
        src = src.at[:, pl.ds(pl.multiple_of(head * width, width), width)]
        return src, dst.at[slot], kind, t * 4 + i, slot, target

    def send_piece(kind, t, i):
        src, dst, kind, n, slot, target = piece(kind, t, i)
        remote(src, dst, ex_send.at[kind, n], ex_recv.at[kind, slot], target).start()

    def each_piece(kind, go_remote, go_local):
        for i in (2, 1, 3):
            for t in range(2):
                go_remote(kind, t, i)
        for t in range(2):
            @pl.when(c == t)
            def _():
                go_local(kind, t)

            @pl.when(c != t)
            def _():
                go_remote(kind, t, 0)

    def local_piece(kind, t):
        src, dst, _, _, _, _ = piece(kind, t, 0)
        return pltpu.make_async_copy(src, dst, loc.at[kind])

    def exchange(kind):
        each_piece(kind, send_piece, lambda kind, t: local_piece(kind, t).start())

    def wait_exchange(kind):
        _, dst, _ = kinds[kind]

        def one(i, cc):
            aa = (a + i) % 4
            slot = 2 * aa + cc
            remote(dst.at[slot], dst.at[slot], ex_send.at[kind, 0], ex_recv.at[kind, slot], dev_ab(aa, b, z, cc)).wait_recv()

        for i in range(1, 4):
            for cc in range(2):
                one(i, cc)
        one(0, 1 - c)
        for t in range(2):
            @pl.when(c == t)
            def _():
                local_piece(kind, t).wait()

    HALF = GROUP // 2

    def z_part(kind, way, hop, sub):
        near, far = ((kn, kf), (vn, vf))[kind]
        at = ((0, 4, 3, 2, 1), (0, 1, 2, 0, 1))[way][hop] * GROUP + sub * HALF
        return (near if hop <= 2 else far).at[pl.ds(at, HALF)]

    def z_copy(kind, way, step, sub):
        target = dev(x, y, (z + 1) % NZ if way == 0 else (z + 7) % NZ, c)
        return remote(z_part(kind, way, step - 1, sub), z_part(kind, way, step, sub),
                      z_send.at[kind, way, step - 1, sub], z_recv.at[kind, way, step - 1, sub], target)

    def z_parts(step):
        return [(way, sub) for sub in range(2) for way in range(2) if step < 4 or way == sub]

    def z_first(kind):
        for way, sub in z_parts(1):
            z_copy(kind, way, 1, sub).start()

    def z_hop(kind, step):
        for way, sub in z_parts(step):
            z_copy(kind, way, step, sub).wait_recv()
            if (way, sub) in z_parts(step + 1) and step < 4:
                z_copy(kind, way, step + 1, sub).start()

    up = dev_ab(a, (b + 1) % 4, z, c)
    down = dev_ab(a, (b + 3) % 4, z, c)
    total_u = U[0] + U[1]

    def b_copy(kind, part, n):
        have = (ku, vu)[kind]
        rel = (krl, vrl)[kind]
        u = U[part]
        h = u // 2
        p = 3 * U[0] * part
        f = HELD + p
        l = U[0] * part
        src, dst, target = (
            (pack.at[pl.ds(p, u)], have.at[pl.ds(f, u)], up),
            (pack.at[pl.ds(p + 2 * u, u)], have.at[pl.ds(f + 2 * u, u)], down),
            (pack.at[pl.ds(p + u, h)], rel.at[pl.ds(l, h)], up),
            (pack.at[pl.ds(p + u + h, h)], rel.at[pl.ds(l + h, h)], down),
            (rel.at[pl.ds(l, h)], have.at[pl.ds(f + u, h)], up),
            (rel.at[pl.ds(l + h, h)], have.at[pl.ds(f + u + h, h)], down),
        )[n]
        return remote(src, dst, b_send.at[kind, part, n], b_recv.at[kind, part, n], target)

    def b_begin(kind, part):
        held = ((kn, kf), (vn, vf))[kind][part]
        u = U[part]
        p = 3 * U[0] * part
        base, size = (0, NEAR) if part == 0 else (NEAR, AFAR)

        def one(r, _):
            for j in range(3):
                pack[p + j * u + r] = held[jnp.clip(smem[2, (j + 1) * TW + U[0] * part + r] - base, 0, size - 1)]
            return 0

        lax.fori_loop(0, u, one, 0)
        for n in (2, 3, 0, 1):
            b_copy(kind, part, n).start()

    def b_relay(kind, part):
        for n in (2, 3):
            b_copy(kind, part, n).wait_recv()
            b_copy(kind, part, n + 2).start()

    def b_end(kind, part):
        for n in (0, 1, 4, 5):
            b_copy(kind, part, n).wait_recv()

    def keep(kind, part):
        held = ((kn, kf), (vn, vf))[kind][part]
        at = pl.ds(0, NEAR) if part == 0 else pl.ds(NEAR, AFAR)
        return pltpu.make_async_copy(held, (ku, vu)[kind].at[at], loc.at[9 + 2 * kind + part])

    def b_sent(kind):
        for part in range(2):
            for n in range(6):
                b_copy(kind, part, n).wait_send()

    def near_far(t):
        far = (t // 32 - z + NZ) % NZ
        return (far >= 3) & (far <= 5)

    def lists():
        f32, bf16, i32 = jnp.float32, jnp.bfloat16, jnp.int32
        n = NZ * NY * 2 * NX

        def one(hit):
            return jnp.where(hit, 1.0, 0.0).astype(f32)

        t_lane = lax.broadcasted_iota(i32, (NZ * NY * 2, n), 1)
        slots = slott[...].reshape(NZ * NY * 2, D)
        perm = jnp.concatenate([one(slots[:, h : h + 1] == t_lane) for h in range(NX)], axis=0).astype(bf16)
        keys = keyt[...].reshape(n, D)
        lane = lax.broadcasted_iota(i32, (n, D), 1)
        named = jnp.concatenate([one(keys == lane), one(keys == lane + D)], axis=1).astype(bf16)
        entry = jnp.dot(named, perm, preferred_element_type=f32)
        block = jnp.max(entry.reshape(4 * GROUP, SEL, n), axis=1)
        by_y = jnp.max(block.reshape(NY, GROUP, n), axis=1)
        by_x = functools.reduce(jnp.maximum, [block[i * NX : (i + 1) * NX] for i in range(2 * NY)])
        want = jnp.concatenate([by_y, by_x], axis=0)
        t0 = lax.broadcasted_iota(i32, (n, n), 0)
        t1 = lax.broadcasted_iota(i32, (n, n), 1)
        before = (t0 < t1) & (near_far(t0) == near_far(t1))
        same_y = (t0 // 8) % NY == (t1 // 8) % NY
        same_x = t0 % NX == t1 % NX
        rank_y = jnp.dot(want.astype(bf16), one(before & same_y).astype(bf16), preferred_element_type=f32)
        rank_x = jnp.dot(want.astype(bf16), one(before & same_x).astype(bf16), preferred_element_type=f32)
        group = lax.broadcasted_iota(i32, (8, n), 0)
        t8 = lax.broadcasted_iota(i32, (8, n), 1)
        first = group < 4
        rank = jnp.where(first, rank_y, rank_x)
        away = jnp.where(first, (t8 // 8) % NY, t8 % NX) != group % 4
        room = jnp.where(near_far(t8), U[1], U[0]).astype(f32)
        over = one((want > 0.5) & away & (rank > room - 0.5))
        flags[z] = jnp.broadcast_to(jnp.max(over), (8, D)).astype(i32)
        wants[0] = want
        wants[1] = rank
        t = lax.broadcasted_iota(i32, (1, n), 1)
        tx, ty, tc, tz = t % NX, (t // 8) % NY, (t // 4) % 2, t // 32
        ta = tx * (1 - c) + ty * c
        tb = ty * (1 - c) + tx * c
        off = (tz - z + NZ) % NZ
        local = jnp.where(off <= 2, off, jnp.where(off >= 6, off - 3, off + 2)) * GROUP + 2 * ta + tc
        late = near_far(t)

        def row(d):
            at = pl.ds(4 * c + d, 1)
            return wants[0, at, :], wants[1, at, :].astype(i32)

        _, rk = row(b)
        gap = (b - tb + 4) % 4 - 1
        there = HELD + jnp.where(late, 3 * U[0] + gap * U[1], gap * U[0]) + rk
        at = jnp.clip(jnp.where(tb == b, local, there), 0, HELD + 3 * total_u - 1)
        r8 = lax.broadcasted_iota(i32, (8, n), 0)
        at8 = jnp.broadcast_to(at, (8, n))
        lhs = jnp.where(r8 == 0, at8 // 16, jnp.where(r8 == 1, at8 % 16, 1)).astype(f32).astype(bf16)
        got = lax.dot_general(lhs, entry.astype(bf16), (((1,), (1,)), ((), ())), preferred_element_type=f32)
        picks = []
        k = lax.broadcasted_iota(i32, (TW, n), 0)
        for j in range(4):
            wj, rj = row((b + j) % 4)
            kk = jnp.where((wj > 0.5) & (tb == b), rj + jnp.where(late, U[0], 0), -1)
            picks.append(one(kk == k))
        picks = jnp.concatenate(picks, axis=0).astype(bf16)
        names = jnp.broadcast_to(local, (8, n)).astype(f32).astype(bf16)
        chosen = lax.dot_general(names, picks, (((1,), (1,)), ((), ())), preferred_element_type=f32)
        place = got[0:1] * 16.0 + got[1:2]
        index[0:1, :] = place.astype(i32)
        index[1:2, :] = got[2:3].astype(i32)
        index[2:3, :] = chosen[0:1].astype(i32)

    def to_scalars():
        return pltpu.make_async_copy(index, smem, loc.at[8])

    def entry_at(m):
        aa, cc = m // 2, m % 2
        yy = y * (1 - c) + aa * c
        xx = aa * (1 - c) + x * c
        return ((yy * 2 + cc) * NX + xx) * SEL

    def gather_entries(src, m):
        first = entry_at(m)
        for e in range(SEL):
            cat[e * ROWS : (e + 1) * ROWS, :] = src[jnp.clip(smem[0, first + e], 0, HELD + 3 * total_u - 1)]
        return first

    row = lax.broadcasted_iota(jnp.int32, (2 * ROWS, ROWS), 0) % ROWS
    col = lax.broadcasted_iota(jnp.int32, (2 * ROWS, ROWS), 1)
    seen = col <= row

    def scores(m, _):
        first = gather_entries(ku, m)
        bias = [jnp.where(smem[1, first + e] > 0, 0.0, -jnp.inf).astype(jnp.float32) for e in range(SEL)]

        def heads(h, _):
            two = qbuf[m, :, pl.ds(pl.multiple_of(h * 2 * D, 2 * D), 2 * D)]
            two = jnp.concatenate([two[:, :D], two[:, D:]], axis=0)
            sc = lax.dot_general(two, cat[...], (((1,), (1,)), ((), ())), preferred_element_type=jnp.float32)
            parts = [jnp.where(seen, sc[:, :ROWS], -jnp.inf)]
            parts += [sc[:, e * ROWS : (e + 1) * ROWS] + bias[e] for e in range(1, SEL)]
            top = functools.reduce(jnp.maximum, parts)
            top = jnp.max(top, axis=1, keepdims=True)
            parts = [jnp.exp2((p - top) * SCALE2) for p in parts]
            total = jnp.sum(functools.reduce(jnp.add, parts), axis=1, keepdims=True)
            inv = 1.0 / total
            at = pl.ds(pl.multiple_of(h * 2 * ROWS, 2 * ROWS), 2 * ROWS)
            for e in range(SEL):
                pbuf[m, at, e * ROWS : (e + 1) * ROWS] = (parts[e] * inv).astype(jnp.bfloat16)
            return 0

        lax.fori_loop(0, GQ // 2, heads, 0)
        return 0

    def columns(head):
        return out_ref.at[:, pl.ds(pl.multiple_of(head * GQ * D, GQ * D), GQ * D)]

    def out_copy(i, cc):
        m = 2 * ((a + i) % 4) + cc
        return remote(obuf.at[m], columns(g), o_send.at[2 * i + cc], o_recv.at[g], dev_ab((a + i) % 4, b, z, cc))

    def out_via(cc):
        m = 2 * ((a + 2) % 4) + cc
        step = 1 if cc == 0 else 3
        return remote(obuf.at[m], orl.at[cc], o_send.at[4 + cc], r_recv.at[cc], dev_ab((a + step) % 4, b, z, c))

    def out_relay(cc):
        step = 1 if cc == 0 else 3
        source = (a + 4 - step) % 4 + 4 * c
        return remote(orl.at[cc], columns(source), o_send.at[8 + cc], o_recv.at[source], dev_ab((a + step) % 4, b, z, cc))

    def out_local():
        return pltpu.make_async_copy(obuf.at[2 * a + c], columns(g), loc.at[5])

    def attend(n, _):
        q = n // 2
        i = jnp.where(q < 2, 2 + q, 3 - q)
        cc = n % 2
        m = 2 * ((a + i) % 4) + cc
        gather_entries(vu, m)

        def heads(h, _):
            at = pl.ds(pl.multiple_of(h * 2 * ROWS, 2 * ROWS), 2 * ROWS)
            o = jnp.dot(pbuf[m, at, :], cat[...], preferred_element_type=jnp.float32).astype(jnp.bfloat16)
            first = pl.multiple_of(h * 2 * D, 2 * D)
            obuf[m, :, pl.ds(first, D)] = o[:ROWS]
            obuf[m, :, pl.ds(pl.multiple_of(first + D, D), D)] = o[ROWS:]
            return 0

        lax.fori_loop(0, GQ // 2, heads, 0)
        for k in range(2):
            @pl.when(n == k)
            def _():
                out_via(k).start()
        for q0, i0 in ((1, 3), (2, 1), (3, 0)):
            for k in range(2):
                @pl.when((n == 2 * q0 + k) & ((i0 > 0) | (c != k)))
                def _():
                    out_copy(i0, k).start()

        @pl.when(n == 6 + c)
        def _():
            out_local().start()

        @pl.when(n == 4)
        def _():
            for k in range(2):
                remote(orl.at[k], orl.at[k], o_send.at[4 + k], r_recv.at[k],
                       dev_ab((a + (3 if k == 0 else 1)) % 4, b, z, c)).wait_recv()
                out_relay(k).start()

        return 0

    exchange(0)
    for n in range(1, 8):
        for copy in t_copy(n, False):
            copy.start()
    for copy in t_local():
        copy.start()
    exchange(1)
    exchange(2)
    wait_exchange(0)
    z_first(0)
    for n in range(1, 8):
        for copy in t_copy(n, True):
            copy.wait_recv()
    for copy in t_local():
        copy.wait()
    for n in range(1, 8):
        tz_copy(0, n, False).start()
    z_hop(0, 1)
    for n in range(1, 8):
        tz_copy(0, n, True).wait_recv()
    lists()
    z_hop(0, 2)
    to_scalars().start()
    for n in range(1, 8):
        tz_copy(1, n, False).start()
    to_scalars().wait()
    b_begin(0, 0)
    z_hop(0, 3)
    wait_exchange(1)
    z_first(1)
    b_relay(0, 0)
    z_hop(0, 4)
    keep(0, 0).start()
    keep(0, 1).start()
    b_begin(0, 1)
    z_hop(1, 1)
    b_relay(0, 1)
    z_hop(1, 2)
    b_end(0, 0)
    wait_exchange(2)
    keep(0, 0).wait()
    keep(0, 1).wait()
    b_end(0, 1)
    b_sent(0)
    b_begin(1, 0)
    lax.fori_loop(0, 1, scores, 0)
    z_hop(1, 3)
    b_relay(1, 0)
    lax.fori_loop(1, 3, scores, 0)
    z_hop(1, 4)
    keep(1, 0).start()
    keep(1, 1).start()
    b_begin(1, 1)
    lax.fori_loop(3, 5, scores, 0)
    b_relay(1, 1)
    lax.fori_loop(5, 8, scores, 0)
    b_end(1, 0)
    keep(1, 0).wait()
    keep(1, 1).wait()
    b_end(1, 1)
    lax.fori_loop(0, 8, attend, 0)

    for n in range(1, 8):
        tz_copy(1, n, True).wait_recv()
    flag_ref[...] = functools.reduce(jnp.maximum, [flags[i] for i in range(NZ)])
    for n in range(1, 8):
        for copy in t_copy(n, False):
            copy.wait_send()
        for kind in range(2):
            tz_copy(kind, n, False).wait_send()
    for kind in range(3):
        def sent(kind, t, i):
            src, dst, kind, n, slot, target = piece(kind, t, i)
            remote(src, dst, ex_send.at[kind, n], ex_recv.at[kind, slot], target).wait_send()

        each_piece(kind, sent, lambda kind, t: None)
    for kind in range(2):
        for step in range(1, 5):
            for way, sub in z_parts(step):
                z_copy(kind, way, step, sub).wait_send()
    b_sent(1)
    for k in range(2):
        out_via(k).wait_send()
        out_relay(k).wait_send()
        for i in (1, 3):
            out_copy(i, k).wait_send()

        @pl.when(c != k)
        def _():
            out_copy(0, k).wait_send()
    out_local().wait()
    for h in range(8):
        dst = out_ref.at[:, pl.ds(h * GQ * D, GQ * D)]
        source = dev(h % 4, y, z, 0) if h < 4 else dev(x, h % 4, z, 1)

        @pl.when(g != h)
        def _():
            remote(dst, dst, o_send.at[0], o_recv.at[h], source).wait_recv()


def attention(U, ident, named, slots, queries, keys, values):
    any_space = pl.BlockSpec(memory_space=pl.ANY)
    vmem = pl.BlockSpec(memory_space=pltpu.VMEM)
    block = (ROWS, D)
    bf16 = jnp.bfloat16
    dma = pltpu.SemaphoreType.DMA
    near, far = U
    return pl.pallas_call(
        functools.partial(kernel, U),
        out_shape=(jax.ShapeDtypeStruct(queries.shape, bf16), jax.ShapeDtypeStruct((8, D), jnp.int32)),
        in_specs=[vmem] * 2 + [any_space] * 3,
        out_specs=(any_space, vmem),
        scratch_shapes=[
            pltpu.VMEM((GROUP, ROWS, GQ * D), bf16),
            pltpu.VMEM((NEAR, *block), bf16),
            pltpu.VMEM((AFAR, *block), bf16),
            pltpu.VMEM((NEAR, *block), bf16),
            pltpu.VMEM((AFAR, *block), bf16),
            pltpu.VMEM((HELD + 3 * (near + far), *block), bf16),
            pltpu.VMEM((HELD + 3 * (near + far), *block), bf16),
            pltpu.VMEM((3 * (near + far), *block), bf16),
            pltpu.VMEM((near + far, *block), bf16),
            pltpu.VMEM((near + far, *block), bf16),
            pltpu.VMEM((SEL * ROWS, D), bf16),
            pltpu.VMEM((GROUP, GQ * ROWS, SEL * ROWS), bf16),
            pltpu.VMEM((GROUP, ROWS, GQ * D), bf16),
            pltpu.VMEM((2, ROWS, GQ * D), bf16),
            pltpu.VMEM((8, 4 * SEL, D), jnp.int32),
            pltpu.VMEM((NZ, 8, D), jnp.int32),
            pltpu.VMEM((2, 8, 256), jnp.float32),
            pltpu.VMEM((8, 256), jnp.int32),
            pltpu.SMEM((8, 256), jnp.int32),
            pltpu.VMEM((NZ, 8, D), jnp.int32),
            dma((3, 8)), dma((3, 8)),
            dma((2, 2, 4, 2)), dma((2, 2, 4, 2)),
            dma((2, 2, 6)), dma((2, 2, 6)),
            dma((10,)), dma((8,)), dma((2,)),
            dma((4, 8)), dma((4, 8)),
            dma((13,)),
        ],
        compiler_params=pltpu.CompilerParams(
            collective_id=ident, has_side_effects=True, vmem_limit_bytes=61 * 1024 * 1024),
    )(named, slots, queries, keys, values)


def body(queries, keys, values, selected, counts, block_slot):
    live = jnp.arange(SEL, dtype=jnp.int32)[None, :] < counts[:, None]
    named = jnp.where(live, (selected % NX) * (NZ * NY * 2) + selected // NX, -1)
    named = jnp.broadcast_to(named.reshape(-1, 1), (4 * SEL, D))
    slots = jnp.pad(block_slot, (0, D - 4))[None, :]
    out, flag = attention(FAST, 0, named, slots, queries, keys, values)
    again = lambda: attention(FULL, 1, named, slots, queries, keys, values)[0]
    return lax.cond(flag[0, 0] > 0, again, lambda: out)


def solution(mesh):
    return jax.shard_map(
        body,
        mesh=mesh,
        in_specs=(
            P(("seq", "head"), None),
            P(("seq", "head"), None),
            P(("seq", "head"), None),
            P("seq", None),
            P("seq"),
            P("seq"),
        ),
        out_specs=P(("seq", "head"), None),
        check_vma=False,
    )
```

```python
import functools
import math

import jax
import jax.numpy as jnp
from jax import lax
from jax.experimental import pallas as pl
from jax.experimental.pallas import tpu as pltpu
from jax.sharding import PartitionSpec as P

MESH = pl.DeviceIdType.MESH
ROWS = 128
D = 128
NX, NY, NZ = 4, 4, 8
GROUP = 8
SEL = 8
HELD = NZ * GROUP
GQ = 8
FAST = (10, 6, 8)
CLASSES = FULL = (5 * GROUP, 2 * GROUP, GROUP)
STARTS = (0, CLASSES[0], CLASSES[0] + CLASSES[1])
TW = 64
SCALE2 = math.log2(math.e) / math.sqrt(D)


def kernel(U, sel_ref, count_ref, own_ref, q_ref, k_ref, v_ref, out_ref, flag_ref,
           key_ref, slot_ref, qbuf, kn, km, kf, vn, vm, vf, ku, vu, kpack, vpack, krl, vrl, cat, pbuf, obuf, orl, keyt, slott, wants, index, smem, flags,
           ex_send, ex_recv, z_send, z_recv, b_send, b_recv, o_send, o_recv, r_recv, t_send, t_recv, loc):
    s = lax.axis_index("seq")
    x = lax.axis_index("head")
    c = s % 2
    y = (s // 2) % NY
    z = s // (2 * NY)
    a = x * (1 - c) + y * c
    b = y * (1 - c) + x * c
    g = a + 4 * c
    r0 = y * 2 + c

    def dev(xx, yy, zz, cc):
        return ((zz * NY + yy) * 2 + cc, xx)

    def dev_ab(aa, bb, zz, cc):
        return dev(aa * (1 - c) + bb * c, bb * (1 - c) + aa * c, zz, cc)

    def remote(src, dst, send, recv, target):
        return pltpu.make_async_remote_copy(src_ref=src, dst_ref=dst, send_sem=send, recv_sem=recv,
                                            device_id=target, device_id_type=MESH)

    OFF = (0, U[0], U[0] + U[1])
    total_u = sum(U)

    row = lax.broadcasted_iota(jnp.int32, (4 * SEL, D), 0)
    lane = lax.broadcasted_iota(jnp.int32, (1, D), 1)
    names = jnp.full((4 * SEL, D), -1, jnp.int32)
    spots = jnp.zeros((1, D), jnp.int32)
    for h in range(NX):
        for e in range(SEL):
            block = sel_ref[h, e]
            name = jnp.where(e < count_ref[h], (block % NX) * (NZ * NY * 2) + block // NX, -1)
            names = jnp.where(row == h * SEL + e, name, names)
        spots = jnp.where(lane == h, own_ref[h], spots)
    key_ref[...] = names
    slot_ref[...] = spots

    barrier = pltpu.get_barrier_semaphore()

    def greet(target):
        pl.semaphore_signal(barrier, inc=1, device_id=target, device_id_type=MESH)

    greet(dev(x, y, z, 1 - c))
    for i in range(1, 4):
        for cc in range(2):
            greet(dev((x + i) % NX, y, z, cc))
            greet(dev(x, (y + i) % NY, z, cc))
    for i in range(1, NZ):
        greet(dev(x, y, (z + i) % NZ, c))
    pl.semaphore_wait(barrier, 20)

    def t_copy(n, receive):
        other = (r0 + n) % 8
        row = other if receive else r0
        target = dev(x, other // 2, z, other % 2)
        sem = (8 - n) % 8 if receive else n
        return (
            remote(key_ref, keyt.at[row], t_send.at[0, n], t_recv.at[0, sem], target),
            remote(slot_ref, slott.at[z, pl.ds(row, 1)], t_send.at[1, n], t_recv.at[1, sem], target),
        )

    def tz_copy(kind, n, receive):
        other = (z + n) % NZ
        row = other if receive else z
        sem = (8 - n) % 8 if receive else n
        buf = (slott, flags)[kind]
        return remote(buf.at[row], buf.at[row], t_send.at[2 + kind, n], t_recv.at[2 + kind, sem], dev(x, y, other, c))

    def t_local():
        return (pltpu.make_async_copy(key_ref, keyt.at[r0], loc.at[6]),
                pltpu.make_async_copy(slot_ref, slott.at[z, pl.ds(r0, 1)], loc.at[7]))

    kinds = ((k_ref, kn, D), (v_ref, vn, D), (q_ref, qbuf, GQ * D))

    def piece(kind, t, i):
        src, dst, width = kinds[kind]
        other = (x + i) % NX if t == 0 else (y + i) % NY
        head = other + 4 * t
        slot = (2 * x + c) if t == 0 else (2 * y + c)
        target = dev(other, y, z, 0) if t == 0 else dev(x, other, z, 1)
        src = src.at[:, pl.ds(pl.multiple_of(head * width, width), width)]
        return src, dst.at[slot], kind, t * 4 + i, slot, target

    def send_piece(kind, t, i):
        src, dst, kind, n, slot, target = piece(kind, t, i)
        remote(src, dst, ex_send.at[kind, n], ex_recv.at[kind, slot], target).start()

    def each_piece(kind, go_remote, go_local):
        for i in (2, 1, 3):
            for t in range(2):
                go_remote(kind, t, i)
        for t in range(2):
            @pl.when(c == t)
            def _():
                go_local(kind, t)

            @pl.when(c != t)
            def _():
                go_remote(kind, t, 0)

    def local_piece(kind, t):
        src, dst, _, _, _, _ = piece(kind, t, 0)
        return pltpu.make_async_copy(src, dst, loc.at[kind])

    def exchange(kind):
        each_piece(kind, send_piece, lambda kind, t: local_piece(kind, t).start())

    def wait_exchange(kind):
        _, dst, _ = kinds[kind]

        def one(i, cc):
            aa = (a + i) % 4
            slot = 2 * aa + cc
            remote(dst.at[slot], dst.at[slot], ex_send.at[kind, 0], ex_recv.at[kind, slot], dev_ab(aa, b, z, cc)).wait_recv()

        for i in range(1, 4):
            for cc in range(2):
                one(i, cc)
        one(0, 1 - c)
        for t in range(2):
            @pl.when(c == t)
            def _():
                local_piece(kind, t).wait()

    HALF = GROUP // 2

    def z_part(kind, way, hop, sub):
        bufs = ((kn, km, kf), (vn, vm, vf))[kind]
        at = ((0, 4, 3, 1, 0), (0, 1, 2, 0, 0))[way][hop] * GROUP + sub * HALF
        return bufs[max(hop - 2, 0)].at[pl.ds(at, HALF)]

    def z_copy(kind, way, step, sub):
        target = dev(x, y, (z + 1) % NZ if way == 0 else (z + 7) % NZ, c)
        return remote(z_part(kind, way, step - 1, sub), z_part(kind, way, step, sub),
                      z_send.at[kind, way, step - 1, sub], z_recv.at[kind, way, step - 1, sub], target)

    def z_parts(step):
        return [(way, sub) for sub in range(2) for way in range(2) if step < 4 or way == sub]

    def z_first(kind):
        for way, sub in z_parts(1):
            z_copy(kind, way, 1, sub).start()

    def z_hop(kind, step):
        for way, sub in z_parts(step):
            z_copy(kind, way, step, sub).wait_recv()
            if (way, sub) in z_parts(step + 1) and step < 4:
                z_copy(kind, way, step + 1, sub).start()

    up = dev_ab(a, (b + 1) % 4, z, c)
    down = dev_ab(a, (b + 3) % 4, z, c)

    def b_copy(kind, part, n):
        have = (ku, vu)[kind]
        rel = (krl, vrl)[kind]
        pack = (kpack, vpack)[kind]
        u = U[part]
        h = u // 2
        p = 3 * OFF[part]
        f = HELD + p
        l = OFF[part]
        src, dst, target = (
            (pack.at[pl.ds(p, u)], have.at[pl.ds(f, u)], up),
            (pack.at[pl.ds(p + 2 * u, u)], have.at[pl.ds(f + 2 * u, u)], down),
            (pack.at[pl.ds(p + u, h)], rel.at[pl.ds(l, h)], up),
            (pack.at[pl.ds(p + u + h, h)], rel.at[pl.ds(l + h, h)], down),
            (rel.at[pl.ds(l, h)], have.at[pl.ds(f + u, h)], up),
            (rel.at[pl.ds(l + h, h)], have.at[pl.ds(f + u + h, h)], down),
        )[n]
        return remote(src, dst, b_send.at[kind, part, n], b_recv.at[kind, part, n], target)

    def b_begin(kind, part):
        bufs = ((kn, km, kf), (vn, vm, vf))[kind]
        pack = (kpack, vpack)[kind]
        u = U[part]

        def one(r, _):
            for j in range(3):
                i = smem[2, (j + 1) * TW + OFF[part] + r]
                block = None
                for k in range(part + 1):
                    other = bufs[k][jnp.clip(i - STARTS[k], 0, CLASSES[k] - 1)]
                    block = other if k == 0 else lax.select(i >= STARTS[k], other, block)
                pack[3 * OFF[part] + j * u + r] = block
            return 0

        lax.fori_loop(0, u, one, 0)
        for n in (2, 3, 0, 1):
            b_copy(kind, part, n).start()

    def b_relay(kind, part):
        for n in (2, 3):
            b_copy(kind, part, n).wait_recv()
            b_copy(kind, part, n + 2).start()

    def b_end(kind, part):
        for n in (0, 1, 4, 5):
            b_copy(kind, part, n).wait_recv()

    def keep(kind, part):
        held = ((kn, km, kf), (vn, vm, vf))[kind][part]
        at = pl.ds(STARTS[part], CLASSES[part])
        return pltpu.make_async_copy(held, (ku, vu)[kind].at[at], loc.at[9 + 3 * kind + part])

    def keep_all(kind):
        for part in range(3):
            keep(kind, part).start()

    def kept(kind):
        for part in range(3):
            keep(kind, part).wait()

    def b_sent(kind):
        for part in range(3):
            for n in range(6):
                b_copy(kind, part, n).wait_send()

    def distance_class(t):
        off = (t // 32 - z + NZ) % NZ
        return jnp.where(off == 4, 2, jnp.where((off == 3) | (off == 5), 1, 0))

    def lists():
        f32, bf16, i32 = jnp.float32, jnp.bfloat16, jnp.int32
        n = NZ * NY * 2 * NX

        def one(hit):
            return jnp.where(hit, 1.0, 0.0).astype(f32)

        t_lane = lax.broadcasted_iota(i32, (NZ * NY * 2, n), 1)
        slots = slott[...].reshape(NZ * NY * 2, D)
        perm = jnp.concatenate([one(slots[:, h : h + 1] == t_lane) for h in range(NX)], axis=0).astype(bf16)
        keys = keyt[...].reshape(n, D)
        lane = lax.broadcasted_iota(i32, (n, D), 1)
        named = jnp.concatenate([one(keys == lane), one(keys == lane + D)], axis=1).astype(bf16)
        entry = jnp.dot(named, perm, preferred_element_type=f32)
        block = jnp.max(entry.reshape(4 * GROUP, SEL, n), axis=1)
        by_y = jnp.max(block.reshape(NY, GROUP, n), axis=1)
        by_x = functools.reduce(jnp.maximum, [block[i * NX : (i + 1) * NX] for i in range(2 * NY)])
        want = jnp.concatenate([by_y, by_x], axis=0)
        t0 = lax.broadcasted_iota(i32, (n, n), 0)
        t1 = lax.broadcasted_iota(i32, (n, n), 1)
        class0, class1 = distance_class(t0), distance_class(t1)
        before = (class0 < class1) | ((class0 == class1) & (t0 < t1))
        same_y = (t0 // 8) % NY == (t1 // 8) % NY
        same_x = t0 % NX == t1 % NX
        want_b = want.astype(bf16)

        def count(which):
            return jnp.dot(want_b, one(which).astype(bf16), preferred_element_type=f32)

        group = lax.broadcasted_iota(i32, (8, n), 0)
        t8 = lax.broadcasted_iota(i32, (8, n), 1)
        first = group < 4
        rank = jnp.where(first, count(before & same_y), count(before & same_x))
        n0, n1 = [jnp.where(first, count(same_y & (class0 == k)), count(same_x & (class0 == k))) for k in range(2)]
        away = jnp.where(first, (t8 // 8) % NY, t8 % NX) != group % 4
        class8 = distance_class(t8)
        rank = jnp.where(class8 >= 1, rank + jnp.maximum(U[0] - n0, 0.0), rank)
        rank = jnp.where(class8 == 2, rank + jnp.maximum(OFF[2] - n1 - jnp.maximum(n0, float(U[0])), 0.0), rank)
        over = one((want > 0.5) & away & (rank > total_u - 0.5))
        flags[z] = jnp.broadcast_to(jnp.max(over), (8, D)).astype(i32)
        wants[0] = want
        wants[1] = rank
        t = lax.broadcasted_iota(i32, (1, n), 1)
        tx, ty, tc, tz = t % NX, (t // 8) % NY, (t // 4) % 2, t // 32
        ta = tx * (1 - c) + ty * c
        tb = ty * (1 - c) + tx * c
        off = (tz - z + NZ) % NZ
        spot = jnp.where(off <= 2, off, jnp.where(off >= 6, off - 3, jnp.where(off == 4, 7, jnp.where(off == 3, 5, 6))))
        local = spot * GROUP + 2 * ta + tc

        def row(d):
            at = pl.ds(4 * c + d, 1)
            return wants[0, at, :], wants[1, at, :].astype(i32)

        _, rk = row(b)
        gap = (b - tb + 4) % 4 - 1
        shift = jnp.where(rk >= OFF[2], 2 * OFF[2] + gap * U[2], jnp.where(rk >= U[0], 2 * U[0] + gap * U[1], gap * U[0]))
        there = HELD + rk + shift
        at = jnp.clip(jnp.where(tb == b, local, there), 0, HELD + 3 * total_u - 1)
        r8 = lax.broadcasted_iota(i32, (8, n), 0)
        at8 = jnp.broadcast_to(at, (8, n))
        lhs = jnp.where(r8 == 0, at8 // 16, jnp.where(r8 == 1, at8 % 16, 1)).astype(f32).astype(bf16)
        got = lax.dot_general(lhs, entry.astype(bf16), (((1,), (1,)), ((), ())), preferred_element_type=f32)
        picks = []
        k = lax.broadcasted_iota(i32, (TW, n), 0)
        for j in range(4):
            wj, rj = row((b + j) % 4)
            kk = jnp.where((wj > 0.5) & (tb == b), rj, -1)
            picks.append(one(kk == k))
        picks = jnp.concatenate(picks, axis=0).astype(bf16)
        names = jnp.broadcast_to(local, (8, n)).astype(f32).astype(bf16)
        chosen = lax.dot_general(names, picks, (((1,), (1,)), ((), ())), preferred_element_type=f32)
        place = got[0:1] * 16.0 + got[1:2]
        index[0:1, :] = place.astype(i32)
        index[1:2, :] = got[2:3].astype(i32)
        index[2:3, :] = chosen[0:1].astype(i32)

    def to_scalars():
        return pltpu.make_async_copy(index, smem, loc.at[8])

    def entry_at(m):
        aa, cc = m // 2, m % 2
        yy = y * (1 - c) + aa * c
        xx = aa * (1 - c) + x * c
        return ((yy * 2 + cc) * NX + xx) * SEL

    def gather_entries(src, m):
        first = entry_at(m)
        for e in range(SEL):
            cat[e * ROWS : (e + 1) * ROWS, :] = src[jnp.clip(smem[0, first + e], 0, HELD + 3 * total_u - 1)]
        return first

    row = lax.broadcasted_iota(jnp.int32, (2 * ROWS, ROWS), 0) % ROWS
    col = lax.broadcasted_iota(jnp.int32, (2 * ROWS, ROWS), 1)
    seen = col <= row

    def scores(m, _):
        first = gather_entries(ku, m)
        bias = [jnp.where(smem[1, first + e] > 0, 0.0, -jnp.inf).astype(jnp.float32) for e in range(SEL)]

        def heads(h, _):
            two = qbuf[m, :, pl.ds(pl.multiple_of(h * 2 * D, 2 * D), 2 * D)]
            two = jnp.concatenate([two[:, :D], two[:, D:]], axis=0)
            sc = lax.dot_general(two, cat[...], (((1,), (1,)), ((), ())), preferred_element_type=jnp.float32)
            parts = [jnp.where(seen, sc[:, :ROWS], -jnp.inf)]
            parts += [sc[:, e * ROWS : (e + 1) * ROWS] + bias[e] for e in range(1, SEL)]
            top = functools.reduce(jnp.maximum, parts)
            top = jnp.max(top, axis=1, keepdims=True)
            parts = [jnp.exp2((p - top) * SCALE2) for p in parts]
            total = jnp.sum(functools.reduce(jnp.add, parts), axis=1, keepdims=True)
            inv = 1.0 / total
            at = pl.ds(pl.multiple_of(h * 2 * ROWS, 2 * ROWS), 2 * ROWS)
            for e in range(SEL):
                pbuf[m, at, e * ROWS : (e + 1) * ROWS] = (parts[e] * inv).astype(jnp.bfloat16)
            return 0

        lax.fori_loop(0, GQ // 2, heads, 0, unroll=2)
        return 0

    def columns(head):
        return out_ref.at[:, pl.ds(pl.multiple_of(head * GQ * D, GQ * D), GQ * D)]

    def out_copy(i, cc):
        m = 2 * ((a + i) % 4) + cc
        return remote(obuf.at[m], columns(g), o_send.at[2 * i + cc], o_recv.at[g], dev_ab((a + i) % 4, b, z, cc))

    def out_via(cc):
        m = 2 * ((a + 2) % 4) + cc
        step = 1 if cc == 0 else 3
        return remote(obuf.at[m], orl.at[cc], o_send.at[4 + cc], r_recv.at[cc], dev_ab((a + step) % 4, b, z, c))

    def out_relay(cc):
        step = 1 if cc == 0 else 3
        source = (a + 4 - step) % 4 + 4 * c
        return remote(orl.at[cc], columns(source), o_send.at[8 + cc], o_recv.at[source], dev_ab((a + step) % 4, b, z, cc))

    def out_local():
        return pltpu.make_async_copy(obuf.at[2 * a + c], columns(g), loc.at[5])

    def attend(n, _):
        q = n // 2
        i = jnp.where(q < 2, 2 + q, 3 - q)
        cc = n % 2
        m = 2 * ((a + i) % 4) + cc
        gather_entries(vu, m)

        def heads(h, _):
            at = pl.ds(pl.multiple_of(h * 2 * ROWS, 2 * ROWS), 2 * ROWS)
            o = jnp.dot(pbuf[m, at, :], cat[...], preferred_element_type=jnp.float32).astype(jnp.bfloat16)
            first = pl.multiple_of(h * 2 * D, 2 * D)
            obuf[m, :, pl.ds(first, D)] = o[:ROWS]
            obuf[m, :, pl.ds(pl.multiple_of(first + D, D), D)] = o[ROWS:]
            return 0

        lax.fori_loop(0, GQ // 2, heads, 0, unroll=2)
        for k in range(2):
            @pl.when(n == k)
            def _():
                out_via(k).start()
        for q0, i0 in ((1, 3), (2, 1), (3, 0)):
            for k in range(2):
                @pl.when((n == 2 * q0 + k) & ((i0 > 0) | (c != k)))
                def _():
                    out_copy(i0, k).start()

        @pl.when(n == 6 + c)
        def _():
            out_local().start()

        @pl.when(n == 4)
        def _():
            for k in range(2):
                remote(orl.at[k], orl.at[k], o_send.at[4 + k], r_recv.at[k],
                       dev_ab((a + (3 if k == 0 else 1)) % 4, b, z, c)).wait_recv()
                out_relay(k).start()

        return 0

    exchange(0)
    for n in range(1, 8):
        for copy in t_copy(n, False):
            copy.start()
    for copy in t_local():
        copy.start()
    exchange(1)
    exchange(2)
    wait_exchange(0)
    z_first(0)
    for n in range(1, 8):
        for copy in t_copy(n, True):
            copy.wait_recv()
    for copy in t_local():
        copy.wait()
    for n in range(1, 8):
        tz_copy(0, n, False).start()
    z_hop(0, 1)
    for n in range(1, 8):
        tz_copy(0, n, True).wait_recv()
    lists()
    z_hop(0, 2)
    to_scalars().start()
    for n in range(1, 8):
        tz_copy(1, n, False).start()
    to_scalars().wait()
    b_begin(0, 0)
    z_hop(0, 3)
    b_begin(0, 1)
    b_relay(0, 0)
    wait_exchange(1)
    z_first(1)
    z_hop(0, 4)
    b_begin(0, 2)
    keep_all(0)
    b_relay(0, 1)
    z_hop(1, 1)
    b_relay(0, 2)
    z_hop(1, 2)
    b_begin(1, 0)
    wait_exchange(2)
    b_end(0, 0)
    b_end(0, 1)
    kept(0)
    b_end(0, 2)
    lax.fori_loop(0, 1, scores, 0)
    z_hop(1, 3)
    b_begin(1, 1)
    b_relay(1, 0)
    lax.fori_loop(1, 3, scores, 0)
    b_relay(1, 1)
    z_hop(1, 4)
    b_begin(1, 2)
    keep_all(1)
    lax.fori_loop(3, 5, scores, 0)
    b_relay(1, 2)
    lax.fori_loop(5, 8, scores, 0)
    b_end(1, 0)
    b_end(1, 1)
    kept(1)
    b_end(1, 2)
    lax.fori_loop(0, 8, attend, 0)

    for n in range(1, 8):
        tz_copy(1, n, True).wait_recv()
    flag_ref[0, 0] = jnp.max(functools.reduce(jnp.maximum, [flags[i] for i in range(NZ)]))
    for n in range(1, 8):
        for copy in t_copy(n, False):
            copy.wait_send()
        for kind in range(2):
            tz_copy(kind, n, False).wait_send()
    for kind in range(3):
        def sent(kind, t, i):
            src, dst, kind, n, slot, target = piece(kind, t, i)
            remote(src, dst, ex_send.at[kind, n], ex_recv.at[kind, slot], target).wait_send()

        each_piece(kind, sent, lambda kind, t: None)
    for kind in range(2):
        for step in range(1, 5):
            for way, sub in z_parts(step):
                z_copy(kind, way, step, sub).wait_send()
    b_sent(0)
    b_sent(1)
    for k in range(2):
        out_via(k).wait_send()
        out_relay(k).wait_send()
        for i in (1, 3):
            out_copy(i, k).wait_send()

        @pl.when(c != k)
        def _():
            out_copy(0, k).wait_send()
    out_local().wait()
    for h in range(8):
        dst = out_ref.at[:, pl.ds(h * GQ * D, GQ * D)]
        source = dev(h % 4, y, z, 0) if h < 4 else dev(x, h % 4, z, 1)

        @pl.when(g != h)
        def _():
            remote(dst, dst, o_send.at[0], o_recv.at[h], source).wait_recv()


def attention(U, ident, selected, counts, slots, queries, keys, values):
    any_space = pl.BlockSpec(memory_space=pl.ANY)
    smem = pl.BlockSpec(memory_space=pltpu.SMEM)
    block = (ROWS, D)
    bf16 = jnp.bfloat16
    dma = pltpu.SemaphoreType.DMA
    total = sum(U)
    return pl.pallas_call(
        functools.partial(kernel, U),
        out_shape=(jax.ShapeDtypeStruct(queries.shape, bf16), jax.ShapeDtypeStruct((1, 1), jnp.int32)),
        in_specs=[smem] * 3 + [any_space] * 3,
        out_specs=(any_space, smem),
        scratch_shapes=[
            pltpu.VMEM((4 * SEL, D), jnp.int32),
            pltpu.VMEM((1, D), jnp.int32),
            pltpu.VMEM((GROUP, ROWS, GQ * D), bf16),
            *[pltpu.VMEM((size, *block), bf16) for size in CLASSES * 2],
            pltpu.VMEM((HELD + 3 * total, *block), bf16),
            pltpu.VMEM((HELD + 3 * total, *block), bf16),
            pltpu.VMEM((3 * total, *block), bf16),
            pltpu.VMEM((3 * total, *block), bf16),
            pltpu.VMEM((total, *block), bf16),
            pltpu.VMEM((total, *block), bf16),
            pltpu.VMEM((SEL * ROWS, D), bf16),
            pltpu.VMEM((GROUP, GQ * ROWS, SEL * ROWS), bf16),
            pltpu.VMEM((GROUP, ROWS, GQ * D), bf16),
            pltpu.VMEM((2, ROWS, GQ * D), bf16),
            pltpu.VMEM((8, 4 * SEL, D), jnp.int32),
            pltpu.VMEM((NZ, 8, D), jnp.int32),
            pltpu.VMEM((2, 8, 256), jnp.float32),
            pltpu.VMEM((8, 256), jnp.int32),
            pltpu.SMEM((8, 256), jnp.int32),
            pltpu.VMEM((NZ, 8, D), jnp.int32),
            dma((3, 8)), dma((3, 8)),
            dma((2, 2, 4, 2)), dma((2, 2, 4, 2)),
            dma((2, 3, 6)), dma((2, 3, 6)),
            dma((10,)), dma((8,)), dma((2,)),
            dma((4, 8)), dma((4, 8)),
            dma((15,)),
        ],
        compiler_params=pltpu.CompilerParams(
            collective_id=ident, has_side_effects=True, vmem_limit_bytes=61 * 1024 * 1024),
    )(selected, counts, slots, queries, keys, values)


def body(queries, keys, values, selected, counts, block_slot):
    tables = (selected, counts, block_slot)
    out, flag = attention(FAST, 0, *tables, queries, keys, values)
    again = lambda: attention(FULL, 1, *tables, queries, keys, values)[0]
    return lax.cond(flag[0, 0] > 0, again, lambda: out)


def solution(mesh):
    return jax.shard_map(
        body,
        mesh=mesh,
        in_specs=(
            P(("seq", "head"), None),
            P(("seq", "head"), None),
            P(("seq", "head"), None),
            P("seq", None),
            P("seq"),
            P("seq"),
        ),
        out_specs=P(("seq", "head"), None),
        check_vma=False,
    )
```

```python
import functools
import math

import jax
import jax.numpy as jnp
from jax import lax
from jax.experimental import pallas as pl
from jax.experimental.pallas import tpu as pltpu
from jax.sharding import PartitionSpec as P

MESH = pl.DeviceIdType.MESH
ROWS = 128
D = 128
NX, NY, NZ = 4, 4, 8
GROUP = 8
SEL = 8
HELD = NZ * GROUP
GQ = 8
FAST = (10, 6, 8)
CLASSES = FULL = (5 * GROUP, 2 * GROUP, GROUP)
STARTS = (0, CLASSES[0], CLASSES[0] + CLASSES[1])
TW = 64
SCALE2 = math.log2(math.e) / math.sqrt(D)


def kernel(U, sel_ref, count_ref, own_ref, q_ref, k_ref, v_ref, out_ref, flag_ref,
           key_ref, slot_ref, qbuf, kn, km, kf, vn, vm, vf, ku, vu, kpack, vpack, krl, vrl, cat, pbuf, obuf, orl, keyt, slott, wants, index, smem, flags,
           ex_send, ex_recv, z_send, z_recv, b_send, b_recv, o_send, o_recv, r_recv, t_send, t_recv, loc):
    s = lax.axis_index("seq")
    x = lax.axis_index("head")
    c = s % 2
    y = (s // 2) % NY
    z = s // (2 * NY)
    a = x * (1 - c) + y * c
    b = y * (1 - c) + x * c
    g = a + 4 * c
    r0 = y * 2 + c

    def dev(xx, yy, zz, cc):
        return ((zz * NY + yy) * 2 + cc, xx)

    def dev_ab(aa, bb, zz, cc):
        return dev(aa * (1 - c) + bb * c, bb * (1 - c) + aa * c, zz, cc)

    def remote(src, dst, send, recv, target):
        return pltpu.make_async_remote_copy(src_ref=src, dst_ref=dst, send_sem=send, recv_sem=recv,
                                            device_id=target, device_id_type=MESH)

    OFF = (0, U[0], U[0] + U[1])
    shared = U == FULL
    packs = (kpack, kpack if shared else vpack)
    total_u = sum(U)

    row = lax.broadcasted_iota(jnp.int32, (4 * SEL, D), 0)
    lane = lax.broadcasted_iota(jnp.int32, (1, D), 1)
    names = jnp.full((4 * SEL, D), -1, jnp.int32)
    spots = jnp.zeros((1, D), jnp.int32)
    for h in range(NX):
        for e in range(SEL):
            block = sel_ref[h, e]
            name = jnp.where(e < count_ref[h], (block % NX) * (NZ * NY * 2) + block // NX, -1)
            names = jnp.where(row == h * SEL + e, name, names)
        spots = jnp.where(lane == h, own_ref[h], spots)
    key_ref[...] = names
    slot_ref[...] = spots

    barrier = pltpu.get_barrier_semaphore()

    def greet(target):
        pl.semaphore_signal(barrier, inc=1, device_id=target, device_id_type=MESH)

    greet(dev(x, y, z, 1 - c))
    for i in range(1, 4):
        for cc in range(2):
            greet(dev((x + i) % NX, y, z, cc))
            greet(dev(x, (y + i) % NY, z, cc))
    for i in range(1, NZ):
        greet(dev(x, y, (z + i) % NZ, c))
    pl.semaphore_wait(barrier, 20)

    def t_copy(n, receive):
        other = (r0 + n) % 8
        row = other if receive else r0
        target = dev(x, other // 2, z, other % 2)
        sem = (8 - n) % 8 if receive else n
        return (
            remote(key_ref, keyt.at[row], t_send.at[0, n], t_recv.at[0, sem], target),
            remote(slot_ref, slott.at[z, pl.ds(row, 1)], t_send.at[1, n], t_recv.at[1, sem], target),
        )

    def tz_copy(kind, n, receive):
        other = (z + n) % NZ
        row = other if receive else z
        sem = (8 - n) % 8 if receive else n
        buf = (slott, flags)[kind]
        return remote(buf.at[row], buf.at[row], t_send.at[2 + kind, n], t_recv.at[2 + kind, sem], dev(x, y, other, c))

    def t_local():
        return (pltpu.make_async_copy(key_ref, keyt.at[r0], loc.at[6]),
                pltpu.make_async_copy(slot_ref, slott.at[z, pl.ds(r0, 1)], loc.at[7]))

    kinds = ((k_ref, kn, D), (v_ref, vn, D), (q_ref, qbuf, GQ * D))

    def piece(kind, t, i):
        src, dst, width = kinds[kind]
        other = (x + i) % NX if t == 0 else (y + i) % NY
        head = other + 4 * t
        slot = (2 * x + c) if t == 0 else (2 * y + c)
        target = dev(other, y, z, 0) if t == 0 else dev(x, other, z, 1)
        src = src.at[:, pl.ds(pl.multiple_of(head * width, width), width)]
        return src, dst.at[slot], kind, t * 4 + i, slot, target

    def send_piece(kind, t, i):
        src, dst, kind, n, slot, target = piece(kind, t, i)
        remote(src, dst, ex_send.at[kind, n], ex_recv.at[kind, slot], target).start()

    def each_piece(kind, go_remote, go_local):
        for i in (2, 1, 3):
            for t in range(2):
                go_remote(kind, t, i)
        for t in range(2):
            @pl.when(c == t)
            def _():
                go_local(kind, t)

            @pl.when(c != t)
            def _():
                go_remote(kind, t, 0)

    def local_piece(kind, t):
        src, dst, _, _, _, _ = piece(kind, t, 0)
        return pltpu.make_async_copy(src, dst, loc.at[kind])

    def exchange(kind):
        each_piece(kind, send_piece, lambda kind, t: local_piece(kind, t).start())

    def wait_exchange(kind):
        _, dst, _ = kinds[kind]

        def one(i, cc):
            aa = (a + i) % 4
            slot = 2 * aa + cc
            remote(dst.at[slot], dst.at[slot], ex_send.at[kind, 0], ex_recv.at[kind, slot], dev_ab(aa, b, z, cc)).wait_recv()

        for i in range(1, 4):
            for cc in range(2):
                one(i, cc)
        one(0, 1 - c)
        for t in range(2):
            @pl.when(c == t)
            def _():
                local_piece(kind, t).wait()

    HALF = GROUP // 2

    def z_part(kind, way, hop, sub):
        bufs = ((kn, km, kf), (vn, vm, vf))[kind]
        at = ((0, 4, 3, 1, 0), (0, 1, 2, 0, 0))[way][hop] * GROUP + sub * HALF
        return bufs[max(hop - 2, 0)].at[pl.ds(at, HALF)]

    def z_copy(kind, way, step, sub):
        target = dev(x, y, (z + 1) % NZ if way == 0 else (z + 7) % NZ, c)
        return remote(z_part(kind, way, step - 1, sub), z_part(kind, way, step, sub),
                      z_send.at[kind, way, step - 1, sub], z_recv.at[kind, way, step - 1, sub], target)

    def z_parts(step):
        return [(way, sub) for sub in range(2) for way in range(2) if step < 4 or way == sub]

    def z_first(kind):
        for way, sub in z_parts(1):
            z_copy(kind, way, 1, sub).start()

    def z_hop(kind, step):
        for way, sub in z_parts(step):
            z_copy(kind, way, step, sub).wait_recv()
            if (way, sub) in z_parts(step + 1) and step < 4:
                z_copy(kind, way, step + 1, sub).start()

    up = dev_ab(a, (b + 1) % 4, z, c)
    down = dev_ab(a, (b + 3) % 4, z, c)

    def b_copy(kind, part, n):
        have = (ku, vu)[kind]
        rel = (krl, vrl)[kind]
        pack = packs[kind]
        u = U[part]
        h = u // 2
        p = 3 * OFF[part]
        f = HELD + p
        l = OFF[part]
        src, dst, target = (
            (pack.at[pl.ds(p, u)], have.at[pl.ds(f, u)], up),
            (pack.at[pl.ds(p + 2 * u, u)], have.at[pl.ds(f + 2 * u, u)], down),
            (pack.at[pl.ds(p + u, h)], rel.at[pl.ds(l, h)], up),
            (pack.at[pl.ds(p + u + h, h)], rel.at[pl.ds(l + h, h)], down),
            (rel.at[pl.ds(l, h)], have.at[pl.ds(f + u, h)], up),
            (rel.at[pl.ds(l + h, h)], have.at[pl.ds(f + u + h, h)], down),
        )[n]
        return remote(src, dst, b_send.at[kind, part, n], b_recv.at[kind, part, n], target)

    def b_begin(kind, part):
        bufs = ((kn, km, kf), (vn, vm, vf))[kind]
        pack = packs[kind]
        u = U[part]

        def one(r, _):
            for j in range(3):
                i = smem[2, (j + 1) * TW + OFF[part] + r]
                block = None
                for k in range(part + 1):
                    other = bufs[k][jnp.clip(i - STARTS[k], 0, CLASSES[k] - 1)]
                    block = other if k == 0 else lax.select(i >= STARTS[k], other, block)
                pack[3 * OFF[part] + j * u + r] = block
            return 0

        lax.fori_loop(0, u, one, 0)
        for n in (2, 3, 0, 1):
            b_copy(kind, part, n).start()

    def b_relay(kind, part):
        for n in (2, 3):
            b_copy(kind, part, n).wait_recv()
            b_copy(kind, part, n + 2).start()

    def b_end(kind, part):
        for n in (0, 1, 4, 5):
            b_copy(kind, part, n).wait_recv()

    def keep(kind, part):
        held = ((kn, km, kf), (vn, vm, vf))[kind][part]
        at = pl.ds(STARTS[part], CLASSES[part])
        return pltpu.make_async_copy(held, (ku, vu)[kind].at[at], loc.at[9 + 3 * kind + part])

    def keep_all(kind):
        for part in range(3):
            keep(kind, part).start()

    def kept(kind):
        for part in range(3):
            keep(kind, part).wait()

    def b_sent(kind):
        for part in range(3):
            for n in range(6):
                b_copy(kind, part, n).wait_send()

    def distance_class(t):
        off = (t // 32 - z + NZ) % NZ
        return jnp.where(off == 4, 2, jnp.where((off == 3) | (off == 5), 1, 0))

    def lists():
        f32, bf16, i32 = jnp.float32, jnp.bfloat16, jnp.int32
        n = NZ * NY * 2 * NX

        def one(hit):
            return jnp.where(hit, 1.0, 0.0).astype(f32)

        t_lane = lax.broadcasted_iota(i32, (NZ * NY * 2, n), 1)
        slots = slott[...].reshape(NZ * NY * 2, D)
        perm = jnp.concatenate([one(slots[:, h : h + 1] == t_lane) for h in range(NX)], axis=0).astype(bf16)
        keys = keyt[...].reshape(n, D)
        lane = lax.broadcasted_iota(i32, (n, D), 1)
        named = jnp.concatenate([one(keys == lane), one(keys == lane + D)], axis=1).astype(bf16)
        entry = jnp.dot(named, perm, preferred_element_type=f32)
        block = jnp.max(entry.reshape(4 * GROUP, SEL, n), axis=1)
        by_y = jnp.max(block.reshape(NY, GROUP, n), axis=1)
        by_x = functools.reduce(jnp.maximum, [block[i * NX : (i + 1) * NX] for i in range(2 * NY)])
        want = jnp.concatenate([by_y, by_x], axis=0)
        t0 = lax.broadcasted_iota(i32, (n, n), 0)
        t1 = lax.broadcasted_iota(i32, (n, n), 1)
        class0, class1 = distance_class(t0), distance_class(t1)
        before = (class0 < class1) | ((class0 == class1) & (t0 < t1))
        same_y = (t0 // 8) % NY == (t1 // 8) % NY
        same_x = t0 % NX == t1 % NX
        want_b = want.astype(bf16)

        def count(which):
            return jnp.dot(want_b, one(which).astype(bf16), preferred_element_type=f32)

        group = lax.broadcasted_iota(i32, (8, n), 0)
        t8 = lax.broadcasted_iota(i32, (8, n), 1)
        first = group < 4
        rank = jnp.where(first, count(before & same_y), count(before & same_x))
        n0, n1 = [jnp.where(first, count(same_y & (class0 == k)), count(same_x & (class0 == k))) for k in range(2)]
        away = jnp.where(first, (t8 // 8) % NY, t8 % NX) != group % 4
        class8 = distance_class(t8)
        rank = jnp.where(class8 >= 1, rank + jnp.maximum(U[0] - n0, 0.0), rank)
        rank = jnp.where(class8 == 2, rank + jnp.maximum(OFF[2] - n1 - jnp.maximum(n0, float(U[0])), 0.0), rank)
        over = one((want > 0.5) & away & (rank > total_u - 0.5))
        flags[z] = jnp.broadcast_to(jnp.max(over), (8, D)).astype(i32)
        wants[0] = want
        wants[1] = rank
        t = lax.broadcasted_iota(i32, (1, n), 1)
        tx, ty, tc, tz = t % NX, (t // 8) % NY, (t // 4) % 2, t // 32
        ta = tx * (1 - c) + ty * c
        tb = ty * (1 - c) + tx * c
        off = (tz - z + NZ) % NZ
        spot = jnp.where(off <= 2, off, jnp.where(off >= 6, off - 3, jnp.where(off == 4, 7, jnp.where(off == 3, 5, 6))))
        local = spot * GROUP + 2 * ta + tc

        def row(d):
            at = pl.ds(4 * c + d, 1)
            return wants[0, at, :], wants[1, at, :].astype(i32)

        _, rk = row(b)
        gap = (b - tb + 4) % 4 - 1
        shift = jnp.where(rk >= OFF[2], 2 * OFF[2] + gap * U[2], jnp.where(rk >= U[0], 2 * U[0] + gap * U[1], gap * U[0]))
        there = HELD + rk + shift
        at = jnp.clip(jnp.where(tb == b, local, there), 0, HELD + 3 * total_u - 1)
        r8 = lax.broadcasted_iota(i32, (8, n), 0)
        at8 = jnp.broadcast_to(at, (8, n))
        lhs = jnp.where(r8 == 0, at8 // 16, jnp.where(r8 == 1, at8 % 16, 1)).astype(f32).astype(bf16)
        got = lax.dot_general(lhs, entry.astype(bf16), (((1,), (1,)), ((), ())), preferred_element_type=f32)
        picks = []
        k = lax.broadcasted_iota(i32, (TW, n), 0)
        for j in range(4):
            wj, rj = row((b + j) % 4)
            kk = jnp.where((wj > 0.5) & (tb == b), rj, -1)
            picks.append(one(kk == k))
        picks = jnp.concatenate(picks, axis=0).astype(bf16)
        names = jnp.broadcast_to(local, (8, n)).astype(f32).astype(bf16)
        chosen = lax.dot_general(names, picks, (((1,), (1,)), ((), ())), preferred_element_type=f32)
        place = got[0:1] * 16.0 + got[1:2]
        index[0:1, :] = place.astype(i32)
        index[1:2, :] = got[2:3].astype(i32)
        index[2:3, :] = chosen[0:1].astype(i32)

    def to_scalars():
        return pltpu.make_async_copy(index, smem, loc.at[8])

    def entry_at(m):
        aa, cc = m // 2, m % 2
        yy = y * (1 - c) + aa * c
        xx = aa * (1 - c) + x * c
        return ((yy * 2 + cc) * NX + xx) * SEL

    def gather_entries(src, m):
        first = entry_at(m)
        for e in range(SEL):
            cat[e * ROWS : (e + 1) * ROWS, :] = src[jnp.clip(smem[0, first + e], 0, HELD + 3 * total_u - 1)]
        return first

    row = lax.broadcasted_iota(jnp.int32, (2 * ROWS, ROWS), 0) % ROWS
    col = lax.broadcasted_iota(jnp.int32, (2 * ROWS, ROWS), 1)
    seen = col <= row

    def scores(m, _):
        first = gather_entries(ku, m)
        bias = [jnp.where(smem[1, first + e] > 0, 0.0, -jnp.inf).astype(jnp.float32) for e in range(SEL)]

        def heads(h, _):
            two = qbuf[m, :, pl.ds(pl.multiple_of(h * 2 * D, 2 * D), 2 * D)]
            two = jnp.concatenate([two[:, :D], two[:, D:]], axis=0)
            sc = lax.dot_general(two, cat[...], (((1,), (1,)), ((), ())), preferred_element_type=jnp.float32)
            parts = [jnp.where(seen, sc[:, :ROWS], -jnp.inf)]
            parts += [sc[:, e * ROWS : (e + 1) * ROWS] + bias[e] for e in range(1, SEL)]
            top = functools.reduce(jnp.maximum, parts)
            top = jnp.max(top, axis=1, keepdims=True)
            parts = [jnp.exp2((p - top) * SCALE2) for p in parts]
            total = jnp.sum(functools.reduce(jnp.add, parts), axis=1, keepdims=True)
            inv = 1.0 / total
            at = pl.ds(pl.multiple_of(h * 2 * ROWS, 2 * ROWS), 2 * ROWS)
            for e in range(SEL):
                pbuf[m, at, e * ROWS : (e + 1) * ROWS] = (parts[e] * inv).astype(jnp.bfloat16)
            return 0

        lax.fori_loop(0, GQ // 2, heads, 0, unroll=2)
        return 0

    def columns(head):
        return out_ref.at[:, pl.ds(pl.multiple_of(head * GQ * D, GQ * D), GQ * D)]

    def out_copy(i, cc):
        m = 2 * ((a + i) % 4) + cc
        return remote(obuf.at[m], columns(g), o_send.at[2 * i + cc], o_recv.at[g], dev_ab((a + i) % 4, b, z, cc))

    def out_via(cc):
        m = 2 * ((a + 2) % 4) + cc
        step = 1 if cc == 0 else 3
        return remote(obuf.at[m], orl.at[cc], o_send.at[4 + cc], r_recv.at[cc], dev_ab((a + step) % 4, b, z, c))

    def out_relay(cc):
        step = 1 if cc == 0 else 3
        source = (a + 4 - step) % 4 + 4 * c
        return remote(orl.at[cc], columns(source), o_send.at[8 + cc], o_recv.at[source], dev_ab((a + step) % 4, b, z, cc))

    def out_local():
        return pltpu.make_async_copy(obuf.at[2 * a + c], columns(g), loc.at[5])

    def attend(n, _):
        q = n // 2
        i = jnp.where(q == 0, 2, jnp.where(q == 3, 0, 1 + 2 * (n % 2)))
        cc = jnp.where((q == 0) | (q == 3), n % 2, q - 1)
        m = 2 * ((a + i) % 4) + cc
        gather_entries(vu, m)

        def heads(h, _):
            at = pl.ds(pl.multiple_of(h * 2 * ROWS, 2 * ROWS), 2 * ROWS)
            o = jnp.dot(pbuf[m, at, :], cat[...], preferred_element_type=jnp.float32).astype(jnp.bfloat16)
            first = pl.multiple_of(h * 2 * D, 2 * D)
            obuf[m, :, pl.ds(first, D)] = o[:ROWS]
            obuf[m, :, pl.ds(pl.multiple_of(first + D, D), D)] = o[ROWS:]
            return 0

        lax.fori_loop(0, GQ // 2, heads, 0, unroll=2)
        for k in range(2):
            @pl.when(n == k)
            def _():
                out_via(k).start()
        for k in range(4):
            @pl.when(n == 2 + k)
            def _():
                out_copy(1 + 2 * (k % 2), k // 2).start()
        for k in range(2):
            @pl.when((n == 6 + k) & (c != k))
            def _():
                out_copy(0, k).start()

        @pl.when(n == 6 + c)
        def _():
            out_local().start()

        for k in range(2):
            @pl.when(n == 5 + k)
            def _():
                remote(orl.at[k], orl.at[k], o_send.at[4 + k], r_recv.at[k],
                       dev_ab((a + (3 if k == 0 else 1)) % 4, b, z, c)).wait_recv()
                out_relay(k).start()

        return 0

    exchange(0)
    for n in range(1, 8):
        for copy in t_copy(n, False):
            copy.start()
    for copy in t_local():
        copy.start()
    exchange(1)
    exchange(2)
    wait_exchange(0)
    z_first(0)
    for n in range(1, 8):
        for copy in t_copy(n, True):
            copy.wait_recv()
    for copy in t_local():
        copy.wait()
    for n in range(1, 8):
        tz_copy(0, n, False).start()
    z_hop(0, 1)
    for n in range(1, 8):
        tz_copy(0, n, True).wait_recv()
    lists()
    z_hop(0, 2)
    to_scalars().start()
    for n in range(1, 8):
        tz_copy(1, n, False).start()
    to_scalars().wait()
    b_begin(0, 0)
    z_hop(0, 3)
    b_begin(0, 1)
    b_relay(0, 0)
    wait_exchange(1)
    z_first(1)
    z_hop(0, 4)
    b_begin(0, 2)
    keep_all(0)
    b_relay(0, 1)
    z_hop(1, 1)
    b_relay(0, 2)
    z_hop(1, 2)
    if shared:
        b_sent(0)
    b_begin(1, 0)
    wait_exchange(2)
    b_end(0, 0)
    b_end(0, 1)
    kept(0)
    b_end(0, 2)
    lax.fori_loop(0, 2, scores, 0)
    z_hop(1, 3)
    b_begin(1, 1)
    b_relay(1, 0)
    lax.fori_loop(2, 4, scores, 0)
    z_hop(1, 4)
    b_begin(1, 2)
    keep_all(1)
    b_relay(1, 1)
    lax.fori_loop(4, 6, scores, 0)
    b_relay(1, 2)
    lax.fori_loop(6, 8, scores, 0)
    b_end(1, 0)
    b_end(1, 1)
    kept(1)
    b_end(1, 2)
    lax.fori_loop(0, 8, attend, 0)

    for n in range(1, 8):
        tz_copy(1, n, True).wait_recv()
    flag_ref[0, 0] = jnp.max(functools.reduce(jnp.maximum, [flags[i] for i in range(NZ)]))
    for n in range(1, 8):
        for copy in t_copy(n, False):
            copy.wait_send()
        for kind in range(2):
            tz_copy(kind, n, False).wait_send()
    for kind in range(3):
        def sent(kind, t, i):
            src, dst, kind, n, slot, target = piece(kind, t, i)
            remote(src, dst, ex_send.at[kind, n], ex_recv.at[kind, slot], target).wait_send()

        each_piece(kind, sent, lambda kind, t: None)
    for kind in range(2):
        for step in range(1, 5):
            for way, sub in z_parts(step):
                z_copy(kind, way, step, sub).wait_send()
    if not shared:
        b_sent(0)
    b_sent(1)
    for k in range(2):
        out_via(k).wait_send()
        out_relay(k).wait_send()
        for i in (1, 3):
            out_copy(i, k).wait_send()

        @pl.when(c != k)
        def _():
            out_copy(0, k).wait_send()
    out_local().wait()
    for h in range(8):
        dst = out_ref.at[:, pl.ds(h * GQ * D, GQ * D)]
        source = dev(h % 4, y, z, 0) if h < 4 else dev(x, h % 4, z, 1)

        @pl.when(g != h)
        def _():
            remote(dst, dst, o_send.at[0], o_recv.at[h], source).wait_recv()


def attention(U, ident, selected, counts, slots, queries, keys, values):
    any_space = pl.BlockSpec(memory_space=pl.ANY)
    smem = pl.BlockSpec(memory_space=pltpu.SMEM)
    block = (ROWS, D)
    bf16 = jnp.bfloat16
    dma = pltpu.SemaphoreType.DMA
    total = sum(U)
    return pl.pallas_call(
        functools.partial(kernel, U),
        out_shape=(pltpu.VMEM(queries.shape, bf16), jax.ShapeDtypeStruct((1, 1), jnp.int32)),
        in_specs=[smem] * 3 + [any_space] * 3,
        out_specs=(pl.BlockSpec(memory_space=pltpu.VMEM), smem),
        scratch_shapes=[
            pltpu.VMEM((4 * SEL, D), jnp.int32),
            pltpu.VMEM((1, D), jnp.int32),
            pltpu.VMEM((GROUP, ROWS, GQ * D), bf16),
            *[pltpu.VMEM((size, *block), bf16) for size in CLASSES * 2],
            pltpu.VMEM((HELD + 3 * total, *block), bf16),
            pltpu.VMEM((HELD + 3 * total, *block), bf16),
            pltpu.VMEM((3 * total, *block), bf16),
            pltpu.VMEM((1 if U == FULL else 3 * total, *block), bf16),
            pltpu.VMEM((total, *block), bf16),
            pltpu.VMEM((total, *block), bf16),
            pltpu.VMEM((SEL * ROWS, D), bf16),
            pltpu.VMEM((GROUP, GQ * ROWS, SEL * ROWS), bf16),
            pltpu.VMEM((GROUP, ROWS, GQ * D), bf16),
            pltpu.VMEM((2, ROWS, GQ * D), bf16),
            pltpu.VMEM((8, 4 * SEL, D), jnp.int32),
            pltpu.VMEM((NZ, 8, D), jnp.int32),
            pltpu.VMEM((2, 8, 256), jnp.float32),
            pltpu.VMEM((8, 256), jnp.int32),
            pltpu.SMEM((8, 256), jnp.int32),
            pltpu.VMEM((NZ, 8, D), jnp.int32),
            dma((3, 8)), dma((3, 8)),
            dma((2, 2, 4, 2)), dma((2, 2, 4, 2)),
            dma((2, 3, 6)), dma((2, 3, 6)),
            dma((10,)), dma((8,)), dma((2,)),
            dma((4, 8)), dma((4, 8)),
            dma((15,)),
        ],
        compiler_params=pltpu.CompilerParams(
            collective_id=ident, has_side_effects=True, vmem_limit_bytes=(58 if U == FULL else 44) * 1024 * 1024),
    )(selected, counts, slots, queries, keys, values)


def body(queries, keys, values, selected, counts, block_slot):
    tables = (selected, counts, block_slot)
    out, flag = attention(FAST, 0, *tables, queries, keys, values)
    again = lambda: attention(FULL, 1, *tables, queries, keys, values)[0]
    return lax.cond(flag[0, 0] > 0, again, lambda: out)


def solution(mesh):
    return jax.shard_map(
        body,
        mesh=mesh,
        in_specs=(
            P(("seq", "head"), None),
            P(("seq", "head"), None),
            P(("seq", "head"), None),
            P("seq", None),
            P("seq"),
            P("seq"),
        ),
        out_specs=P(("seq", "head"), None),
        check_vma=False,
    )
```

```python
import functools
import math

import jax
import jax.numpy as jnp
from jax import lax
from jax.experimental import pallas as pl
from jax.experimental.pallas import tpu as pltpu
from jax.sharding import PartitionSpec as P

MESH = pl.DeviceIdType.MESH
ROWS = 128
D = 128
NX, NY, NZ = 4, 4, 8
GROUP = 8
SEL = 8
HELD = NZ * GROUP
GQ = 8
FAST = (10, 6, 8)
CLASSES = FULL = (5 * GROUP, 2 * GROUP, GROUP)
STARTS = (0, CLASSES[0], CLASSES[0] + CLASSES[1])
TW = 64
SCALE2 = math.log2(math.e) / math.sqrt(D)


def kernel(U, sel_ref, count_ref, own_ref, q_ref, k_ref, v_ref, out_ref, flag_ref,
           key_ref, slot_ref, qbuf, kn, km, kf, vn, vm, vf, ku, vu, kpack, vpack, krl, vrl, cat, pbuf, obuf, orl, keyt, slott, wants, index, smem, flags,
           ex_send, ex_recv, z_send, z_recv, b_send, b_recv, o_send, o_recv, r_recv, t_send, t_recv, loc):
    s = lax.axis_index("seq")
    x = lax.axis_index("head")
    c = s % 2
    y = (s // 2) % NY
    z = s // (2 * NY)
    a = x * (1 - c) + y * c
    b = y * (1 - c) + x * c
    g = a + 4 * c
    r0 = y * 2 + c

    def dev(xx, yy, zz, cc):
        return ((zz * NY + yy) * 2 + cc, xx)

    def dev_ab(aa, bb, zz, cc):
        return dev(aa * (1 - c) + bb * c, bb * (1 - c) + aa * c, zz, cc)

    def remote(src, dst, send, recv, target):
        return pltpu.make_async_remote_copy(src_ref=src, dst_ref=dst, send_sem=send, recv_sem=recv,
                                            device_id=target, device_id_type=MESH)

    OFF = (0, U[0], U[0] + U[1])
    shared = U == FULL
    packs = (kpack, kpack if shared else vpack)
    total_u = sum(U)

    row = lax.broadcasted_iota(jnp.int32, (4 * SEL, D), 0)
    lane = lax.broadcasted_iota(jnp.int32, (1, D), 1)
    names = jnp.full((4 * SEL, D), -1, jnp.int32)
    spots = jnp.zeros((1, D), jnp.int32)
    for h in range(NX):
        for e in range(SEL):
            block = sel_ref[h, e]
            name = jnp.where(e < count_ref[h], (block % NX) * (NZ * NY * 2) + block // NX, -1)
            names = jnp.where(row == h * SEL + e, name, names)
        spots = jnp.where(lane == h, own_ref[h], spots)
    key_ref[...] = names
    slot_ref[...] = spots

    barrier = pltpu.get_barrier_semaphore()

    def greet(target):
        pl.semaphore_signal(barrier, inc=1, device_id=target, device_id_type=MESH)

    greet(dev(x, y, z, 1 - c))
    for i in range(1, 4):
        for cc in range(2):
            greet(dev((x + i) % NX, y, z, cc))
            greet(dev(x, (y + i) % NY, z, cc))
    for i in range(1, NZ):
        greet(dev(x, y, (z + i) % NZ, c))
    pl.semaphore_wait(barrier, 20)

    def t_copy(n, receive):
        other = (r0 + n) % 8
        row = other if receive else r0
        target = dev(x, other // 2, z, other % 2)
        sem = (8 - n) % 8 if receive else n
        return (
            remote(key_ref, keyt.at[row], t_send.at[0, n], t_recv.at[0, sem], target),
            remote(slot_ref, slott.at[z, pl.ds(row, 1)], t_send.at[1, n], t_recv.at[1, sem], target),
        )

    def tz_copy(kind, n, receive):
        other = (z + n) % NZ
        row = other if receive else z
        sem = (8 - n) % 8 if receive else n
        buf = (slott, flags)[kind]
        return remote(buf.at[row], buf.at[row], t_send.at[2 + kind, n], t_recv.at[2 + kind, sem], dev(x, y, other, c))

    def t_local():
        return (pltpu.make_async_copy(key_ref, keyt.at[r0], loc.at[6]),
                pltpu.make_async_copy(slot_ref, slott.at[z, pl.ds(r0, 1)], loc.at[7]))

    kinds = ((k_ref, kn, D), (v_ref, vn, D), (q_ref, qbuf, GQ * D))

    def piece(kind, t, i):
        src, dst, width = kinds[kind]
        other = (x + i) % NX if t == 0 else (y + i) % NY
        head = other + 4 * t
        slot = (2 * x + c) if t == 0 else (2 * y + c)
        target = dev(other, y, z, 0) if t == 0 else dev(x, other, z, 1)
        src = src.at[:, pl.ds(pl.multiple_of(head * width, width), width)]
        return src, dst.at[slot], kind, t * 4 + i, slot, target

    def send_piece(kind, t, i):
        src, dst, kind, n, slot, target = piece(kind, t, i)
        remote(src, dst, ex_send.at[kind, n], ex_recv.at[kind, slot], target).start()

    def each_piece(kind, go_remote, go_local):
        for i in (2, 1, 3):
            for t in range(2):
                go_remote(kind, t, i)
        for t in range(2):
            @pl.when(c == t)
            def _():
                go_local(kind, t)

            @pl.when(c != t)
            def _():
                go_remote(kind, t, 0)

    def local_piece(kind, t):
        src, dst, _, _, _, _ = piece(kind, t, 0)
        return pltpu.make_async_copy(src, dst, loc.at[kind])

    def exchange(kind):
        each_piece(kind, send_piece, lambda kind, t: local_piece(kind, t).start())

    def wait_exchange(kind, places=(0, 1, 3, 2)):
        _, dst, _ = kinds[kind]

        def one(i, cc):
            aa = (a + i) % 4
            slot = 2 * aa + cc
            remote(dst.at[slot], dst.at[slot], ex_send.at[kind, 0], ex_recv.at[kind, slot], dev_ab(aa, b, z, cc)).wait_recv()

        for i in places:
            if i:
                for cc in range(2):
                    one(i, cc)
            else:
                one(0, 1 - c)
                for t in range(2):
                    @pl.when(c == t)
                    def _():
                        local_piece(kind, t).wait()

    def z_part(kind, way, hop, sub):
        bufs = ((kn, km, kf), (vn, vm, vf))[kind]
        at = ((0, 4, 3, 1, 0), (0, 1, 2, 0, 0))[way][hop] * GROUP + 2 * ((a + sub) % 4)
        return bufs[max(hop - 2, 0)].at[pl.ds(at, 2)]

    def z_copy(kind, way, step, sub):
        target = dev(x, y, (z + 1) % NZ if way == 0 else (z + 7) % NZ, c)
        return remote(z_part(kind, way, step - 1, sub), z_part(kind, way, step, sub),
                      z_send.at[kind, way, step - 1, sub], z_recv.at[kind, way, step - 1, sub], target)

    def z_parts(step):
        return [(way, sub) for sub in (0, 1, 3, 2) for way in range(2) if step < 4 or way == sub // 2]

    def z_first(kind):
        for sub in (0, 1, 3, 2):
            wait_exchange(kind, (sub,))
            for way in range(2):
                z_copy(kind, way, 1, sub).start()

    def z_hop(kind, step):
        for way, sub in z_parts(step):
            z_copy(kind, way, step, sub).wait_recv()
            if (way, sub) in z_parts(step + 1) and step < 4:
                z_copy(kind, way, step + 1, sub).start()

    up = dev_ab(a, (b + 1) % 4, z, c)
    down = dev_ab(a, (b + 3) % 4, z, c)

    def b_copy(kind, part, n):
        have = (ku, vu)[kind]
        rel = (krl, vrl)[kind]
        pack = packs[kind]
        u = U[part]
        h = u // 2
        p = 3 * OFF[part]
        f = HELD + p
        l = OFF[part]
        src, dst, target = (
            (pack.at[pl.ds(p, u)], have.at[pl.ds(f, u)], up),
            (pack.at[pl.ds(p + 2 * u, u)], have.at[pl.ds(f + 2 * u, u)], down),
            (pack.at[pl.ds(p + u, h)], rel.at[pl.ds(l, h)], up),
            (pack.at[pl.ds(p + u + h, h)], rel.at[pl.ds(l + h, h)], down),
            (rel.at[pl.ds(l, h)], have.at[pl.ds(f + u, h)], up),
            (rel.at[pl.ds(l + h, h)], have.at[pl.ds(f + u + h, h)], down),
        )[n]
        return remote(src, dst, b_send.at[kind, part, n], b_recv.at[kind, part, n], target)

    def b_begin(kind, part):
        bufs = ((kn, km, kf), (vn, vm, vf))[kind]
        pack = packs[kind]
        u = U[part]

        def one(r, _):
            for j in range(3):
                i = smem[2, (j + 1) * TW + OFF[part] + r]
                block = None
                for k in range(part + 1):
                    other = bufs[k][jnp.clip(i - STARTS[k], 0, CLASSES[k] - 1)]
                    block = other if k == 0 else lax.select(i >= STARTS[k], other, block)
                pack[3 * OFF[part] + j * u + r] = block
            return 0

        lax.fori_loop(0, u, one, 0)
        for n in (2, 3, 0, 1):
            b_copy(kind, part, n).start()

    def b_relay(kind, part):
        for n in (2, 3):
            b_copy(kind, part, n).wait_recv()
            b_copy(kind, part, n + 2).start()

    def b_end(kind, part):
        for n in (0, 1, 4, 5):
            b_copy(kind, part, n).wait_recv()

    def keep(kind, part):
        held = ((kn, km, kf), (vn, vm, vf))[kind][part]
        at = pl.ds(STARTS[part], CLASSES[part])
        return pltpu.make_async_copy(held, (ku, vu)[kind].at[at], loc.at[9 + 3 * kind + part])

    def keep_all(kind):
        for part in range(3):
            keep(kind, part).start()

    def kept(kind):
        for part in range(3):
            keep(kind, part).wait()

    def b_sent(kind):
        for part in range(3):
            for n in range(6):
                b_copy(kind, part, n).wait_send()

    def distance_class(t):
        off = (t // 32 - z + NZ) % NZ
        return jnp.where(off == 4, 2, jnp.where((off == 3) | (off == 5), 1, 0))

    def lists():
        f32, bf16, i32 = jnp.float32, jnp.bfloat16, jnp.int32
        n = NZ * NY * 2 * NX

        def one(hit):
            return jnp.where(hit, 1.0, 0.0).astype(f32)

        t_lane = lax.broadcasted_iota(i32, (NZ * NY * 2, n), 1)
        slots = slott[...].reshape(NZ * NY * 2, D)
        perm = jnp.concatenate([one(slots[:, h : h + 1] == t_lane) for h in range(NX)], axis=0).astype(bf16)
        keys = keyt[...].reshape(n, D)
        lane = lax.broadcasted_iota(i32, (n, D), 1)
        named = jnp.concatenate([one(keys == lane), one(keys == lane + D)], axis=1).astype(bf16)
        entry = jnp.dot(named, perm, preferred_element_type=f32)
        block = jnp.max(entry.reshape(4 * GROUP, SEL, n), axis=1)
        by_y = jnp.max(block.reshape(NY, GROUP, n), axis=1)
        by_x = functools.reduce(jnp.maximum, [block[i * NX : (i + 1) * NX] for i in range(2 * NY)])
        want = jnp.concatenate([by_y, by_x], axis=0)
        t0 = lax.broadcasted_iota(i32, (n, n), 0)
        t1 = lax.broadcasted_iota(i32, (n, n), 1)
        class0, class1 = distance_class(t0), distance_class(t1)
        before = (class0 < class1) | ((class0 == class1) & (t0 < t1))
        same_y = (t0 // 8) % NY == (t1 // 8) % NY
        same_x = t0 % NX == t1 % NX
        want_b = want.astype(bf16)

        def count(which):
            return jnp.dot(want_b, one(which).astype(bf16), preferred_element_type=f32)

        group = lax.broadcasted_iota(i32, (8, n), 0)
        t8 = lax.broadcasted_iota(i32, (8, n), 1)
        first = group < 4
        rank = jnp.where(first, count(before & same_y), count(before & same_x))
        n0, n1 = [jnp.where(first, count(same_y & (class0 == k)), count(same_x & (class0 == k))) for k in range(2)]
        away = jnp.where(first, (t8 // 8) % NY, t8 % NX) != group % 4
        class8 = distance_class(t8)
        rank = jnp.where(class8 >= 1, rank + jnp.maximum(U[0] - n0, 0.0), rank)
        rank = jnp.where(class8 == 2, rank + jnp.maximum(OFF[2] - n1 - jnp.maximum(n0, float(U[0])), 0.0), rank)
        over = one((want > 0.5) & away & (rank > total_u - 0.5))
        flags[z] = jnp.broadcast_to(jnp.max(over), (8, D)).astype(i32)
        wants[0] = want
        wants[1] = rank
        t = lax.broadcasted_iota(i32, (1, n), 1)
        tx, ty, tc, tz = t % NX, (t // 8) % NY, (t // 4) % 2, t // 32
        ta = tx * (1 - c) + ty * c
        tb = ty * (1 - c) + tx * c
        off = (tz - z + NZ) % NZ
        spot = jnp.where(off <= 2, off, jnp.where(off >= 6, off - 3, jnp.where(off == 4, 7, jnp.where(off == 3, 5, 6))))
        local = spot * GROUP + 2 * ta + tc

        def row(d):
            at = pl.ds(4 * c + d, 1)
            return wants[0, at, :], wants[1, at, :].astype(i32)

        _, rk = row(b)
        gap = (b - tb + 4) % 4 - 1
        shift = jnp.where(rk >= OFF[2], 2 * OFF[2] + gap * U[2], jnp.where(rk >= U[0], 2 * U[0] + gap * U[1], gap * U[0]))
        there = HELD + rk + shift
        at = jnp.clip(jnp.where(tb == b, local, there), 0, HELD + 3 * total_u - 1)
        r8 = lax.broadcasted_iota(i32, (8, n), 0)
        at8 = jnp.broadcast_to(at, (8, n))
        lhs = jnp.where(r8 == 0, at8 // 16, jnp.where(r8 == 1, at8 % 16, 1)).astype(f32).astype(bf16)
        got = lax.dot_general(lhs, entry.astype(bf16), (((1,), (1,)), ((), ())), preferred_element_type=f32)
        picks = []
        k = lax.broadcasted_iota(i32, (TW, n), 0)
        for j in range(4):
            wj, rj = row((b + j) % 4)
            kk = jnp.where((wj > 0.5) & (tb == b), rj, -1)
            picks.append(one(kk == k))
        picks = jnp.concatenate(picks, axis=0).astype(bf16)
        names = jnp.broadcast_to(local, (8, n)).astype(f32).astype(bf16)
        chosen = lax.dot_general(names, picks, (((1,), (1,)), ((), ())), preferred_element_type=f32)
        place = got[0:1] * 16.0 + got[1:2]
        index[0:1, :] = place.astype(i32)
        index[1:2, :] = got[2:3].astype(i32)
        index[2:3, :] = chosen[0:1].astype(i32)

    def to_scalars():
        return pltpu.make_async_copy(index, smem, loc.at[8])

    def entry_at(m):
        aa, cc = m // 2, m % 2
        yy = y * (1 - c) + aa * c
        xx = aa * (1 - c) + x * c
        return ((yy * 2 + cc) * NX + xx) * SEL

    def gather_entries(src, m):
        first = entry_at(m)
        for e in range(SEL):
            cat[e * ROWS : (e + 1) * ROWS, :] = src[jnp.clip(smem[0, first + e], 0, HELD + 3 * total_u - 1)]
        return first

    row = lax.broadcasted_iota(jnp.int32, (2 * ROWS, ROWS), 0) % ROWS
    col = lax.broadcasted_iota(jnp.int32, (2 * ROWS, ROWS), 1)
    seen = col <= row

    def scores(m, _):
        first = gather_entries(ku, m)
        bias = [jnp.where(smem[1, first + e] > 0, 0.0, -jnp.inf).astype(jnp.float32) for e in range(SEL)]

        def heads(h, _):
            two = qbuf[m, :, pl.ds(pl.multiple_of(h * 2 * D, 2 * D), 2 * D)]
            two = jnp.concatenate([two[:, :D], two[:, D:]], axis=0)
            sc = lax.dot_general(two, cat[...], (((1,), (1,)), ((), ())), preferred_element_type=jnp.float32)
            parts = [jnp.where(seen, sc[:, :ROWS], -jnp.inf)]
            parts += [sc[:, e * ROWS : (e + 1) * ROWS] + bias[e] for e in range(1, SEL)]
            top = functools.reduce(jnp.maximum, parts)
            top = jnp.max(top, axis=1, keepdims=True)
            parts = [jnp.exp2((p - top) * SCALE2) for p in parts]
            total = jnp.sum(functools.reduce(jnp.add, parts), axis=1, keepdims=True)
            inv = 1.0 / total
            at = pl.ds(pl.multiple_of(h * 2 * ROWS, 2 * ROWS), 2 * ROWS)
            for e in range(SEL):
                pbuf[m, at, e * ROWS : (e + 1) * ROWS] = (parts[e] * inv).astype(jnp.bfloat16)
            return 0

        lax.fori_loop(0, GQ // 2, heads, 0, unroll=2)
        return 0

    def columns(head):
        return out_ref.at[:, pl.ds(pl.multiple_of(head * GQ * D, GQ * D), GQ * D)]

    def out_copy(i, cc):
        m = 2 * ((a + i) % 4) + cc
        return remote(obuf.at[m], columns(g), o_send.at[2 * i + cc], o_recv.at[g], dev_ab((a + i) % 4, b, z, cc))

    def out_via(cc):
        m = 2 * ((a + 2) % 4) + cc
        step = 1 if cc == 0 else 3
        return remote(obuf.at[m], orl.at[cc], o_send.at[4 + cc], r_recv.at[cc], dev_ab((a + step) % 4, b, z, c))

    def out_relay(cc):
        step = 1 if cc == 0 else 3
        source = (a + 4 - step) % 4 + 4 * c
        return remote(orl.at[cc], columns(source), o_send.at[8 + cc], o_recv.at[source], dev_ab((a + step) % 4, b, z, cc))

    def out_local():
        return pltpu.make_async_copy(obuf.at[2 * a + c], columns(g), loc.at[5])

    def attend(n, _):
        q = n // 2
        i = jnp.where(q == 0, 2, jnp.where(q == 3, 0, 1 + 2 * (n % 2)))
        cc = jnp.where((q == 0) | (q == 3), n % 2, q - 1)
        m = 2 * ((a + i) % 4) + cc
        gather_entries(vu, m)

        def heads(h, _):
            at = pl.ds(pl.multiple_of(h * 2 * ROWS, 2 * ROWS), 2 * ROWS)
            o = jnp.dot(pbuf[m, at, :], cat[...], preferred_element_type=jnp.float32).astype(jnp.bfloat16)
            first = pl.multiple_of(h * 2 * D, 2 * D)
            obuf[m, :, pl.ds(first, D)] = o[:ROWS]
            obuf[m, :, pl.ds(pl.multiple_of(first + D, D), D)] = o[ROWS:]
            return 0

        lax.fori_loop(0, GQ // 2, heads, 0, unroll=2)
        for k in range(2):
            @pl.when(n == k)
            def _():
                out_via(k).start()
        for k in range(4):
            @pl.when(n == 2 + k)
            def _():
                out_copy(1 + 2 * (k % 2), k // 2).start()
        for k in range(2):
            @pl.when((n == 6 + k) & (c != k))
            def _():
                out_copy(0, k).start()

        @pl.when(n == 6 + c)
        def _():
            out_local().start()

        for k in range(2):
            @pl.when(n == 5 + k)
            def _():
                remote(orl.at[k], orl.at[k], o_send.at[4 + k], r_recv.at[k],
                       dev_ab((a + (3 if k == 0 else 1)) % 4, b, z, c)).wait_recv()
                out_relay(k).start()

        return 0

    exchange(0)
    for n in range(1, 8):
        for copy in t_copy(n, False):
            copy.start()
    for copy in t_local():
        copy.start()
    exchange(1)
    z_first(0)
    exchange(2)
    for n in range(1, 8):
        for copy in t_copy(n, True):
            copy.wait_recv()
    for copy in t_local():
        copy.wait()
    for n in range(1, 8):
        tz_copy(0, n, False).start()
    z_hop(0, 1)
    z_hop(0, 2)
    for n in range(1, 8):
        tz_copy(0, n, True).wait_recv()
    lists()
    to_scalars().start()
    for n in range(1, 8):
        tz_copy(1, n, False).start()
    to_scalars().wait()
    b_begin(0, 0)
    z_hop(0, 3)
    b_begin(0, 1)
    b_relay(0, 0)
    z_first(1)
    z_hop(0, 4)
    b_begin(0, 2)
    keep_all(0)
    b_relay(0, 1)
    z_hop(1, 1)
    b_relay(0, 2)
    z_hop(1, 2)
    if shared:
        b_sent(0)
    b_begin(1, 0)
    wait_exchange(2)
    b_end(0, 0)
    b_end(0, 1)
    kept(0)
    b_end(0, 2)
    lax.fori_loop(0, 2, scores, 0)
    z_hop(1, 3)
    b_begin(1, 1)
    b_relay(1, 0)
    lax.fori_loop(2, 4, scores, 0)
    z_hop(1, 4)
    b_begin(1, 2)
    keep_all(1)
    b_relay(1, 1)
    lax.fori_loop(4, 6, scores, 0)
    b_relay(1, 2)
    lax.fori_loop(6, 8, scores, 0)
    b_end(1, 0)
    b_end(1, 1)
    kept(1)
    b_end(1, 2)
    lax.fori_loop(0, 8, attend, 0)

    for n in range(1, 8):
        tz_copy(1, n, True).wait_recv()
    flag_ref[0, 0] = jnp.max(functools.reduce(jnp.maximum, [flags[i] for i in range(NZ)]))
    for n in range(1, 8):
        for copy in t_copy(n, False):
            copy.wait_send()
        for kind in range(2):
            tz_copy(kind, n, False).wait_send()
    for kind in range(3):
        def sent(kind, t, i):
            src, dst, kind, n, slot, target = piece(kind, t, i)
            remote(src, dst, ex_send.at[kind, n], ex_recv.at[kind, slot], target).wait_send()

        each_piece(kind, sent, lambda kind, t: None)
    for kind in range(2):
        for step in range(1, 5):
            for way, sub in z_parts(step):
                z_copy(kind, way, step, sub).wait_send()
    if not shared:
        b_sent(0)
    b_sent(1)
    for k in range(2):
        out_via(k).wait_send()
        out_relay(k).wait_send()
        for i in (1, 3):
            out_copy(i, k).wait_send()

        @pl.when(c != k)
        def _():
            out_copy(0, k).wait_send()
    out_local().wait()
    for h in range(8):
        dst = out_ref.at[:, pl.ds(h * GQ * D, GQ * D)]
        source = dev(h % 4, y, z, 0) if h < 4 else dev(x, h % 4, z, 1)

        @pl.when(g != h)
        def _():
            remote(dst, dst, o_send.at[0], o_recv.at[h], source).wait_recv()


def attention(U, ident, selected, counts, slots, queries, keys, values):
    any_space = pl.BlockSpec(memory_space=pl.ANY)
    smem = pl.BlockSpec(memory_space=pltpu.SMEM)
    block = (ROWS, D)
    bf16 = jnp.bfloat16
    dma = pltpu.SemaphoreType.DMA
    total = sum(U)
    return pl.pallas_call(
        functools.partial(kernel, U),
        out_shape=(pltpu.VMEM(queries.shape, bf16), jax.ShapeDtypeStruct((1, 1), jnp.int32)),
        in_specs=[smem] * 3 + [any_space] * 3,
        out_specs=(pl.BlockSpec(memory_space=pltpu.VMEM), smem),
        scratch_shapes=[
            pltpu.VMEM((4 * SEL, D), jnp.int32),
            pltpu.VMEM((1, D), jnp.int32),
            pltpu.VMEM((GROUP, ROWS, GQ * D), bf16),
            *[pltpu.VMEM((size, *block), bf16) for size in CLASSES * 2],
            pltpu.VMEM((HELD + 3 * total, *block), bf16),
            pltpu.VMEM((HELD + 3 * total, *block), bf16),
            pltpu.VMEM((3 * total, *block), bf16),
            pltpu.VMEM((1 if U == FULL else 3 * total, *block), bf16),
            pltpu.VMEM((total, *block), bf16),
            pltpu.VMEM((total, *block), bf16),
            pltpu.VMEM((SEL * ROWS, D), bf16),
            pltpu.VMEM((GROUP, GQ * ROWS, SEL * ROWS), bf16),
            pltpu.VMEM((GROUP, ROWS, GQ * D), bf16),
            pltpu.VMEM((2, ROWS, GQ * D), bf16),
            pltpu.VMEM((8, 4 * SEL, D), jnp.int32),
            pltpu.VMEM((NZ, 8, D), jnp.int32),
            pltpu.VMEM((2, 8, 256), jnp.float32),
            pltpu.VMEM((8, 256), jnp.int32),
            pltpu.SMEM((8, 256), jnp.int32),
            pltpu.VMEM((NZ, 8, D), jnp.int32),
            dma((3, 8)), dma((3, 8)),
            dma((2, 2, 4, 4)), dma((2, 2, 4, 4)),
            dma((2, 3, 6)), dma((2, 3, 6)),
            dma((10,)), dma((8,)), dma((2,)),
            dma((4, 8)), dma((4, 8)),
            dma((15,)),
        ],
        compiler_params=pltpu.CompilerParams(
            collective_id=ident, has_side_effects=True, vmem_limit_bytes=(58 if U == FULL else 44) * 1024 * 1024),
    )(selected, counts, slots, queries, keys, values)


def body(queries, keys, values, selected, counts, block_slot):
    tables = (selected, counts, block_slot)
    out, flag = attention(FAST, 0, *tables, queries, keys, values)
    again = lambda: attention(FULL, 1, *tables, queries, keys, values)[0]
    return lax.cond(flag[0, 0] > 0, again, lambda: out)


def solution(mesh):
    return jax.shard_map(
        body,
        mesh=mesh,
        in_specs=(
            P(("seq", "head"), None),
            P(("seq", "head"), None),
            P(("seq", "head"), None),
            P("seq", None),
            P("seq"),
            P("seq"),
        ),
        out_specs=P(("seq", "head"), None),
        check_vma=False,
    )
```

```python
import functools
import math

import jax
import jax.numpy as jnp
from jax import lax
from jax.experimental import pallas as pl
from jax.experimental.pallas import tpu as pltpu
from jax.sharding import PartitionSpec as P

MESH = pl.DeviceIdType.MESH
ROWS = 128
D = 128
NX, NY, NZ = 4, 4, 8
GROUP = 8
SEL = 8
HELD = NZ * GROUP
GQ = 8
FAST = (10, 6, 8)
CLASSES = FULL = (5 * GROUP, 2 * GROUP, GROUP)
STARTS = (0, CLASSES[0], CLASSES[0] + CLASSES[1])
TW = 64
SCALE2 = math.log2(math.e) / math.sqrt(D)


def kernel(U, sel_ref, count_ref, own_ref, q_ref, k_ref, v_ref, out_ref, flag_ref,
           key_ref, slot_ref, qbuf, kn, km, kf, vn, vm, vf, ku, vu, kpack, vpack, krl, vrl, cat, pbuf, obuf, orl, keyt, slott, wants, index, smem, flags,
           ex_send, ex_recv, z_send, z_recv, b_send, b_recv, o_send, o_recv, r_recv, t_send, t_recv, loc):
    s = lax.axis_index("seq")
    x = lax.axis_index("head")
    c = s % 2
    y = (s // 2) % NY
    z = s // (2 * NY)
    a = x * (1 - c) + y * c
    b = y * (1 - c) + x * c
    g = a + 4 * c
    r0 = y * 2 + c

    def dev(xx, yy, zz, cc):
        return ((zz * NY + yy) * 2 + cc, xx)

    def dev_ab(aa, bb, zz, cc):
        return dev(aa * (1 - c) + bb * c, bb * (1 - c) + aa * c, zz, cc)

    def remote(src, dst, send, recv, target):
        return pltpu.make_async_remote_copy(src_ref=src, dst_ref=dst, send_sem=send, recv_sem=recv,
                                            device_id=target, device_id_type=MESH)

    OFF = (0, U[0], U[0] + U[1])
    shared = U == FULL
    packs = (kpack, kpack if shared else vpack)
    total_u = sum(U)

    row = lax.broadcasted_iota(jnp.int32, (4 * SEL, D), 0)
    lane = lax.broadcasted_iota(jnp.int32, (1, D), 1)
    names = jnp.full((4 * SEL, D), -1, jnp.int32)
    spots = jnp.zeros((1, D), jnp.int32)
    for h in range(NX):
        for e in range(SEL):
            block = sel_ref[h, e]
            name = jnp.where(e < count_ref[h], (block % NX) * (NZ * NY * 2) + block // NX, -1)
            names = jnp.where(row == h * SEL + e, name, names)
        spots = jnp.where(lane == h, own_ref[h], spots)
    key_ref[...] = names
    slot_ref[...] = spots

    barrier = pltpu.get_barrier_semaphore()

    def greet(target):
        pl.semaphore_signal(barrier, inc=1, device_id=target, device_id_type=MESH)

    greet(dev(x, y, z, 1 - c))
    for i in range(1, 4):
        for cc in range(2):
            greet(dev((x + i) % NX, y, z, cc))
            greet(dev(x, (y + i) % NY, z, cc))
    for i in range(1, NZ):
        greet(dev(x, y, (z + i) % NZ, c))
    pl.semaphore_wait(barrier, 20)

    def t_copy(n, receive):
        other = (r0 + n) % 8
        row = other if receive else r0
        target = dev(x, other // 2, z, other % 2)
        sem = (8 - n) % 8 if receive else n
        return (
            remote(key_ref, keyt.at[row], t_send.at[0, n], t_recv.at[0, sem], target),
            remote(slot_ref, slott.at[z, pl.ds(row, 1)], t_send.at[1, n], t_recv.at[1, sem], target),
        )

    def tz_copy(kind, n, receive):
        other = (z + n) % NZ
        row = other if receive else z
        sem = (8 - n) % 8 if receive else n
        buf = (slott, flags)[kind]
        return remote(buf.at[row], buf.at[row], t_send.at[2 + kind, n], t_recv.at[2 + kind, sem], dev(x, y, other, c))

    def t_local():
        return (pltpu.make_async_copy(key_ref, keyt.at[r0], loc.at[6]),
                pltpu.make_async_copy(slot_ref, slott.at[z, pl.ds(r0, 1)], loc.at[7]))

    kinds = ((k_ref, kn, D), (v_ref, vn, D), (q_ref, qbuf, GQ * D))

    def piece(kind, t, i):
        src, dst, width = kinds[kind]
        other = (x + i) % NX if t == 0 else (y + i) % NY
        head = other + 4 * t
        slot = (2 * x + c) if t == 0 else (2 * y + c)
        target = dev(other, y, z, 0) if t == 0 else dev(x, other, z, 1)
        src = src.at[:, pl.ds(pl.multiple_of(head * width, width), width)]
        return src, dst.at[slot], kind, t * 4 + i, slot, target

    def send_piece(kind, t, i):
        src, dst, kind, n, slot, target = piece(kind, t, i)
        remote(src, dst, ex_send.at[kind, n], ex_recv.at[kind, slot], target).start()

    def each_piece(kind, go_remote, go_local):
        for i in (2, 1, 3):
            for t in range(2):
                go_remote(kind, t, i)
        for t in range(2):
            @pl.when(c == t)
            def _():
                go_local(kind, t)

            @pl.when(c != t)
            def _():
                go_remote(kind, t, 0)

    def local_piece(kind, t):
        src, dst, _, _, _, _ = piece(kind, t, 0)
        return pltpu.make_async_copy(src, dst, loc.at[kind])

    def exchange(kind):
        each_piece(kind, send_piece, lambda kind, t: local_piece(kind, t).start())

    def wait_exchange(kind, places=(0, 1, 3, 2)):
        _, dst, _ = kinds[kind]

        def one(i, cc):
            aa = (a + i) % 4
            slot = 2 * aa + cc
            remote(dst.at[slot], dst.at[slot], ex_send.at[kind, 0], ex_recv.at[kind, slot], dev_ab(aa, b, z, cc)).wait_recv()

        for i in places:
            if i:
                for cc in range(2):
                    one(i, cc)
            else:
                one(0, 1 - c)
                for t in range(2):
                    @pl.when(c == t)
                    def _():
                        local_piece(kind, t).wait()

    def z_part(kind, way, hop, sub):
        bufs = ((kn, km, kf), (vn, vm, vf))[kind]
        at = ((0, 4, 3, 1, 0), (0, 1, 2, 0, 0))[way][hop] * GROUP + 2 * ((a + sub) % 4)
        return bufs[max(hop - 2, 0)].at[pl.ds(at, 2)]

    def z_copy(kind, way, step, sub):
        target = dev(x, y, (z + 1) % NZ if way == 0 else (z + 7) % NZ, c)
        return remote(z_part(kind, way, step - 1, sub), z_part(kind, way, step, sub),
                      z_send.at[kind, way, step - 1, sub], z_recv.at[kind, way, step - 1, sub], target)

    def z_parts(step):
        return [(way, sub) for sub in (0, 1, 3, 2) for way in range(2) if step < 4 or way == sub // 2]

    def z_first(kind):
        for sub in (0, 1, 3, 2):
            wait_exchange(kind, (sub,))
            for way in range(2):
                z_copy(kind, way, 1, sub).start()

    def z_hop(kind, step):
        for way, sub in z_parts(step):
            z_copy(kind, way, step, sub).wait_recv()
            if (way, sub) in z_parts(step + 1) and step < 4:
                z_copy(kind, way, step + 1, sub).start()

    up = dev_ab(a, (b + 1) % 4, z, c)
    down = dev_ab(a, (b + 3) % 4, z, c)

    def b_copy(kind, part, n):
        have = (ku, vu)[kind]
        rel = (krl, vrl)[kind]
        pack = packs[kind]
        u = U[part]
        h = u // 2
        p = 3 * OFF[part]
        f = HELD + p
        l = OFF[part]
        src, dst, target = (
            (pack.at[pl.ds(p, u)], have.at[pl.ds(f, u)], up),
            (pack.at[pl.ds(p + 2 * u, u)], have.at[pl.ds(f + 2 * u, u)], down),
            (pack.at[pl.ds(p + u, h)], rel.at[pl.ds(l, h)], up),
            (pack.at[pl.ds(p + u + h, h)], rel.at[pl.ds(l + h, h)], down),
            (rel.at[pl.ds(l, h)], have.at[pl.ds(f + u, h)], up),
            (rel.at[pl.ds(l + h, h)], have.at[pl.ds(f + u + h, h)], down),
        )[n]
        return remote(src, dst, b_send.at[kind, part, n], b_recv.at[kind, part, n], target)

    def b_begin(kind, part):
        bufs = ((kn, km, kf), (vn, vm, vf))[kind]
        pack = packs[kind]
        u = U[part]

        def one(r, _):
            for j in range(3):
                i = smem[2, (j + 1) * TW + OFF[part] + r]
                block = None
                for k in range(part + 1):
                    other = bufs[k][jnp.clip(i - STARTS[k], 0, CLASSES[k] - 1)]
                    block = other if k == 0 else lax.select(i >= STARTS[k], other, block)
                pack[3 * OFF[part] + j * u + r] = block
            return 0

        lax.fori_loop(0, u, one, 0)
        for n in (2, 3, 0, 1):
            b_copy(kind, part, n).start()

    def b_relay(kind, part):
        for n in (2, 3):
            b_copy(kind, part, n).wait_recv()
            b_copy(kind, part, n + 2).start()

    def b_end(kind, part):
        for n in (0, 1, 4, 5):
            b_copy(kind, part, n).wait_recv()

    def keep(kind, part):
        held = ((kn, km, kf), (vn, vm, vf))[kind][part]
        at = pl.ds(STARTS[part], CLASSES[part])
        return pltpu.make_async_copy(held, (ku, vu)[kind].at[at], loc.at[9 + 3 * kind + part])

    def keep_all(kind):
        for part in range(3):
            keep(kind, part).start()

    def kept(kind):
        for part in range(3):
            keep(kind, part).wait()

    def b_sent(kind):
        for part in range(3):
            for n in range(6):
                b_copy(kind, part, n).wait_send()

    def distance_class(t):
        off = (t // 32 - z + NZ) % NZ
        return jnp.where(off == 4, 2, jnp.where((off == 3) | (off == 5), 1, 0))

    def lists():
        f32, bf16, i32 = jnp.float32, jnp.bfloat16, jnp.int32
        n = NZ * NY * 2 * NX

        def one(hit):
            return jnp.where(hit, 1.0, 0.0).astype(f32)

        t_lane = lax.broadcasted_iota(i32, (NZ * NY * 2, n), 1)
        slots = slott[...].reshape(NZ * NY * 2, D)
        perm = jnp.concatenate([one(slots[:, h : h + 1] == t_lane) for h in range(NX)], axis=0).astype(bf16)
        keys = keyt[...].reshape(n, D)
        lane = lax.broadcasted_iota(i32, (n, D), 1)
        named = jnp.concatenate([one(keys == lane), one(keys == lane + D)], axis=1).astype(bf16)
        entry = jnp.dot(named, perm, preferred_element_type=f32)
        block = jnp.max(entry.reshape(4 * GROUP, SEL, n), axis=1)
        by_y = jnp.max(block.reshape(NY, GROUP, n), axis=1)
        by_x = functools.reduce(jnp.maximum, [block[i * NX : (i + 1) * NX] for i in range(2 * NY)])
        want = jnp.concatenate([by_y, by_x], axis=0)
        t0 = lax.broadcasted_iota(i32, (n, n), 0)
        t1 = lax.broadcasted_iota(i32, (n, n), 1)
        class0, class1 = distance_class(t0), distance_class(t1)
        before = (class0 < class1) | ((class0 == class1) & (t0 < t1))
        same_y = (t0 // 8) % NY == (t1 // 8) % NY
        same_x = t0 % NX == t1 % NX
        want_b = want.astype(bf16)

        def count(which):
            return jnp.dot(want_b, one(which).astype(bf16), preferred_element_type=f32)

        group = lax.broadcasted_iota(i32, (8, n), 0)
        t8 = lax.broadcasted_iota(i32, (8, n), 1)
        first = group < 4
        rank = jnp.where(first, count(before & same_y), count(before & same_x))
        n0, n1 = [jnp.where(first, count(same_y & (class0 == k)), count(same_x & (class0 == k))) for k in range(2)]
        away = jnp.where(first, (t8 // 8) % NY, t8 % NX) != group % 4
        class8 = distance_class(t8)
        rank = jnp.where(class8 >= 1, rank + jnp.maximum(U[0] - n0, 0.0), rank)
        rank = jnp.where(class8 == 2, rank + jnp.maximum(OFF[2] - n1 - jnp.maximum(n0, float(U[0])), 0.0), rank)
        over = one((want > 0.5) & away & (rank > total_u - 0.5))
        flags[z] = jnp.broadcast_to(jnp.max(over), (8, D)).astype(i32)
        wants[0] = want
        wants[1] = rank
        t = lax.broadcasted_iota(i32, (1, n), 1)
        tx, ty, tc, tz = t % NX, (t // 8) % NY, (t // 4) % 2, t // 32
        ta = tx * (1 - c) + ty * c
        tb = ty * (1 - c) + tx * c
        off = (tz - z + NZ) % NZ
        spot = jnp.where(off <= 2, off, jnp.where(off >= 6, off - 3, jnp.where(off == 4, 7, jnp.where(off == 3, 5, 6))))
        local = spot * GROUP + 2 * ta + tc

        def row(d):
            at = pl.ds(4 * c + d, 1)
            return wants[0, at, :], wants[1, at, :].astype(i32)

        _, rk = row(b)
        gap = (b - tb + 4) % 4 - 1
        shift = jnp.where(rk >= OFF[2], 2 * OFF[2] + gap * U[2], jnp.where(rk >= U[0], 2 * U[0] + gap * U[1], gap * U[0]))
        there = HELD + rk + shift
        at = jnp.clip(jnp.where(tb == b, local, there), 0, HELD + 3 * total_u - 1)
        r8 = lax.broadcasted_iota(i32, (8, n), 0)
        at8 = jnp.broadcast_to(at, (8, n))
        lhs = jnp.where(r8 == 0, at8 // 16, jnp.where(r8 == 1, at8 % 16, 1)).astype(f32).astype(bf16)
        got = lax.dot_general(lhs, entry.astype(bf16), (((1,), (1,)), ((), ())), preferred_element_type=f32)
        picks = []
        k = lax.broadcasted_iota(i32, (TW, n), 0)
        for j in range(4):
            wj, rj = row((b + j) % 4)
            kk = jnp.where((wj > 0.5) & (tb == b), rj, -1)
            picks.append(one(kk == k))
        picks = jnp.concatenate(picks, axis=0).astype(bf16)
        names = jnp.broadcast_to(local, (8, n)).astype(f32).astype(bf16)
        chosen = lax.dot_general(names, picks, (((1,), (1,)), ((), ())), preferred_element_type=f32)
        place = got[0:1] * 16.0 + got[1:2]
        index[0:1, :] = place.astype(i32)
        index[1:2, :] = got[2:3].astype(i32)
        index[2:3, :] = chosen[0:1].astype(i32)

    def to_scalars():
        return pltpu.make_async_copy(index, smem, loc.at[8])

    def entry_at(m):
        aa, cc = m // 2, m % 2
        yy = y * (1 - c) + aa * c
        xx = aa * (1 - c) + x * c
        return ((yy * 2 + cc) * NX + xx) * SEL

    def gather_entries(src, m):
        first = entry_at(m)
        for e in range(SEL):
            cat[e * ROWS : (e + 1) * ROWS, :] = src[jnp.clip(smem[0, first + e], 0, HELD + 3 * total_u - 1)]
        return first

    row = lax.broadcasted_iota(jnp.int32, (2 * ROWS, ROWS), 0) % ROWS
    col = lax.broadcasted_iota(jnp.int32, (2 * ROWS, ROWS), 1)
    seen = col <= row

    def scores(m, _):
        first = gather_entries(ku, m)
        bias = [jnp.where(smem[1, first + e] > 0, 0.0, -jnp.inf).astype(jnp.float32) for e in range(SEL)]

        def heads(h, _):
            two = qbuf[m, :, pl.ds(pl.multiple_of(h * 2 * D, 2 * D), 2 * D)]
            two = jnp.concatenate([two[:, :D], two[:, D:]], axis=0)
            sc = lax.dot_general(two, cat[...], (((1,), (1,)), ((), ())), preferred_element_type=jnp.float32)
            parts = [jnp.where(seen, sc[:, :ROWS], -jnp.inf)]
            parts += [sc[:, e * ROWS : (e + 1) * ROWS] + bias[e] for e in range(1, SEL)]
            top = functools.reduce(jnp.maximum, parts)
            top = jnp.max(top, axis=1, keepdims=True)
            parts = [jnp.exp2((p - top) * SCALE2) for p in parts]
            total = jnp.sum(functools.reduce(jnp.add, parts), axis=1, keepdims=True)
            inv = 1.0 / total
            at = pl.ds(pl.multiple_of(h * 2 * ROWS, 2 * ROWS), 2 * ROWS)
            for e in range(SEL):
                pbuf[m, at, e * ROWS : (e + 1) * ROWS] = (parts[e] * inv).astype(jnp.bfloat16)
            return 0

        lax.fori_loop(0, GQ // 2, heads, 0, unroll=2)
        return 0

    def columns(head):
        return out_ref.at[:, pl.ds(pl.multiple_of(head * GQ * D, GQ * D), GQ * D)]

    WIDE = GQ * D // 2

    def half_columns(head, half):
        return out_ref.at[:, pl.ds(pl.multiple_of(head * GQ * D + half * WIDE, WIDE), WIDE)]

    def out_half(m, half):
        return obuf.at[m, :, pl.ds(half * WIDE, WIDE)]

    def relay_half(cc, half):
        return orl.at[cc, :, pl.ds(half * WIDE, WIDE)]

    def out_copy(i, cc, half):
        m = 2 * ((a + i) % 4) + cc
        return remote(out_half(m, half), half_columns(g, half), o_send.at[2 * i + cc, half], o_recv.at[g, half],
                      dev_ab((a + i) % 4, b, z, cc))

    def out_via(cc, half):
        m = 2 * ((a + 2) % 4) + cc
        step = 1 if cc == 0 else 3
        return remote(out_half(m, half), relay_half(cc, half), o_send.at[4 + cc, half], r_recv.at[cc, half],
                      dev_ab((a + step) % 4, b, z, c))

    def out_relay(cc, half):
        step = 1 if cc == 0 else 3
        source = (a + 4 - step) % 4 + 4 * c
        return remote(relay_half(cc, half), half_columns(source, half), o_send.at[8 + cc, half], o_recv.at[source, half],
                      dev_ab((a + step) % 4, b, z, cc))

    def out_local():
        return pltpu.make_async_copy(obuf.at[2 * a + c], columns(g), loc.at[5])

    def attend(n, _):
        q = n // 2
        i = jnp.where(q == 0, 2, jnp.where(q == 3, 0, 1 + 2 * (n % 2)))
        cc = jnp.where((q == 0) | (q == 3), n % 2, q - 1)
        m = 2 * ((a + i) % 4) + cc
        gather_entries(vu, m)

        def heads(h, _):
            at = pl.ds(pl.multiple_of(h * 2 * ROWS, 2 * ROWS), 2 * ROWS)
            o = jnp.dot(pbuf[m, at, :], cat[...], preferred_element_type=jnp.float32).astype(jnp.bfloat16)
            first = pl.multiple_of(h * 2 * D, 2 * D)
            obuf[m, :, pl.ds(first, D)] = o[:ROWS]
            obuf[m, :, pl.ds(pl.multiple_of(first + D, D), D)] = o[ROWS:]
            return 0

        for half in range(2):
            lax.fori_loop(2 * half, 2 * half + 2, heads, 0, unroll=2)
            for k in range(2):
                @pl.when(n == k)
                def _():
                    out_via(k, half).start()
            for k in range(4):
                @pl.when(n == 2 + k)
                def _():
                    out_copy(1 + 2 * (k % 2), k // 2, half).start()
            for k in range(2):
                @pl.when((n == 6 + k) & (c != k))
                def _():
                    out_copy(0, k, half).start()

        @pl.when(n == 6 + c)
        def _():
            out_local().start()

        for k in range(2):
            @pl.when(n == 5 + k)
            def _():
                for half in range(2):
                    here = relay_half(k, half)
                    remote(here, here, o_send.at[4 + k, half], r_recv.at[k, half],
                           dev_ab((a + (3 if k == 0 else 1)) % 4, b, z, c)).wait_recv()
                    out_relay(k, half).start()

        return 0

    exchange(0)
    for n in range(1, 8):
        for copy in t_copy(n, False):
            copy.start()
    for copy in t_local():
        copy.start()
    exchange(1)
    z_first(0)
    exchange(2)
    for n in range(1, 8):
        for copy in t_copy(n, True):
            copy.wait_recv()
    for copy in t_local():
        copy.wait()
    for n in range(1, 8):
        tz_copy(0, n, False).start()
    z_hop(0, 1)
    z_hop(0, 2)
    for n in range(1, 8):
        tz_copy(0, n, True).wait_recv()
    lists()
    to_scalars().start()
    for n in range(1, 8):
        tz_copy(1, n, False).start()
    to_scalars().wait()
    b_begin(0, 0)
    z_hop(0, 3)
    b_begin(0, 1)
    b_relay(0, 0)
    z_first(1)
    z_hop(0, 4)
    b_begin(0, 2)
    keep_all(0)
    b_relay(0, 1)
    z_hop(1, 1)
    b_relay(0, 2)
    z_hop(1, 2)
    if shared:
        b_sent(0)
    b_begin(1, 0)
    wait_exchange(2)
    b_end(0, 0)
    b_end(0, 1)
    kept(0)
    b_end(0, 2)
    lax.fori_loop(0, 2, scores, 0)
    z_hop(1, 3)
    b_begin(1, 1)
    b_relay(1, 0)
    lax.fori_loop(2, 4, scores, 0)
    z_hop(1, 4)
    b_begin(1, 2)
    keep_all(1)
    b_relay(1, 1)
    lax.fori_loop(4, 6, scores, 0)
    b_relay(1, 2)
    lax.fori_loop(6, 8, scores, 0)
    b_end(1, 0)
    b_end(1, 1)
    kept(1)
    b_end(1, 2)
    lax.fori_loop(0, 8, attend, 0)

    for n in range(1, 8):
        tz_copy(1, n, True).wait_recv()
    flag_ref[0, 0] = jnp.max(functools.reduce(jnp.maximum, [flags[i] for i in range(NZ)]))
    for n in range(1, 8):
        for copy in t_copy(n, False):
            copy.wait_send()
        for kind in range(2):
            tz_copy(kind, n, False).wait_send()
    for kind in range(3):
        def sent(kind, t, i):
            src, dst, kind, n, slot, target = piece(kind, t, i)
            remote(src, dst, ex_send.at[kind, n], ex_recv.at[kind, slot], target).wait_send()

        each_piece(kind, sent, lambda kind, t: None)
    for kind in range(2):
        for step in range(1, 5):
            for way, sub in z_parts(step):
                z_copy(kind, way, step, sub).wait_send()
    if not shared:
        b_sent(0)
    b_sent(1)
    for k in range(2):
        for half in range(2):
            out_via(k, half).wait_send()
            out_relay(k, half).wait_send()
            for i in (1, 3):
                out_copy(i, k, half).wait_send()

            @pl.when(c != k)
            def _():
                out_copy(0, k, half).wait_send()
    out_local().wait()
    for h in range(8):
        source = dev(h % 4, y, z, 0) if h < 4 else dev(x, h % 4, z, 1)

        @pl.when(g != h)
        def _():
            for half in range(2):
                dst = half_columns(h, half)
                remote(dst, dst, o_send.at[0, half], o_recv.at[h, half], source).wait_recv()


def attention(U, ident, selected, counts, slots, queries, keys, values):
    any_space = pl.BlockSpec(memory_space=pl.ANY)
    smem = pl.BlockSpec(memory_space=pltpu.SMEM)
    block = (ROWS, D)
    bf16 = jnp.bfloat16
    dma = pltpu.SemaphoreType.DMA
    total = sum(U)
    return pl.pallas_call(
        functools.partial(kernel, U),
        out_shape=(pltpu.VMEM(queries.shape, bf16), jax.ShapeDtypeStruct((1, 1), jnp.int32)),
        in_specs=[smem] * 3 + [any_space] * 3,
        out_specs=(pl.BlockSpec(memory_space=pltpu.VMEM), smem),
        scratch_shapes=[
            pltpu.VMEM((4 * SEL, D), jnp.int32),
            pltpu.VMEM((1, D), jnp.int32),
            pltpu.VMEM((GROUP, ROWS, GQ * D), bf16),
            *[pltpu.VMEM((size, *block), bf16) for size in CLASSES * 2],
            pltpu.VMEM((HELD + 3 * total, *block), bf16),
            pltpu.VMEM((HELD + 3 * total, *block), bf16),
            pltpu.VMEM((3 * total, *block), bf16),
            pltpu.VMEM((1 if U == FULL else 3 * total, *block), bf16),
            pltpu.VMEM((total, *block), bf16),
            pltpu.VMEM((total, *block), bf16),
            pltpu.VMEM((SEL * ROWS, D), bf16),
            pltpu.VMEM((GROUP, GQ * ROWS, SEL * ROWS), bf16),
            pltpu.VMEM((GROUP, ROWS, GQ * D), bf16),
            pltpu.VMEM((2, ROWS, GQ * D), bf16),
            pltpu.VMEM((8, 4 * SEL, D), jnp.int32),
            pltpu.VMEM((NZ, 8, D), jnp.int32),
            pltpu.VMEM((2, 8, 256), jnp.float32),
            pltpu.VMEM((8, 256), jnp.int32),
            pltpu.SMEM((8, 256), jnp.int32),
            pltpu.VMEM((NZ, 8, D), jnp.int32),
            dma((3, 8)), dma((3, 8)),
            dma((2, 2, 4, 4)), dma((2, 2, 4, 4)),
            dma((2, 3, 6)), dma((2, 3, 6)),
            dma((10, 2)), dma((8, 2)), dma((2, 2)),
            dma((4, 8)), dma((4, 8)),
            dma((15,)),
        ],
        compiler_params=pltpu.CompilerParams(
            collective_id=ident, has_side_effects=True, vmem_limit_bytes=(58 if U == FULL else 44) * 1024 * 1024),
    )(selected, counts, slots, queries, keys, values)


def body(queries, keys, values, selected, counts, block_slot):
    tables = (selected, counts, block_slot)
    out, flag = attention(FAST, 0, *tables, queries, keys, values)
    again = lambda: attention(FULL, 1, *tables, queries, keys, values)[0]
    return lax.cond(flag[0, 0] > 0, again, lambda: out)


def solution(mesh):
    return jax.shard_map(
        body,
        mesh=mesh,
        in_specs=(
            P(("seq", "head"), None),
            P(("seq", "head"), None),
            P(("seq", "head"), None),
            P("seq", None),
            P("seq"),
            P("seq"),
        ),
        out_specs=P(("seq", "head"), None),
        check_vma=False,
    )
```

```python
import functools
import math

import jax
import jax.numpy as jnp
from jax import lax
from jax.experimental import pallas as pl
from jax.experimental.pallas import tpu as pltpu
from jax.sharding import PartitionSpec as P

MESH = pl.DeviceIdType.MESH
ROWS = 128
D = 128
NX, NY, NZ = 4, 4, 8
GROUP = 8
SEL = 8
HELD = NZ * GROUP
GQ = 8
FAST = (10, 6, 8)
CLASSES = FULL = (5 * GROUP, 2 * GROUP, GROUP)
STARTS = (0, CLASSES[0], CLASSES[0] + CLASSES[1])
TW = 64
SCALE2 = math.log2(math.e) / math.sqrt(D)


def kernel(U, sel_ref, count_ref, own_ref, q_ref, k_ref, v_ref, out_ref, flag_ref,
           key_ref, slot_ref, kin, qbuf, kn, km, kf, vn, vm, vf, ku, vu, kpack, vpack, krl, vrl, cat, pbuf, obuf, orl, keyt, slott, wants, index, smem, flags,
           ex_send, ex_recv, z_send, z_recv, b_send, b_recv, o_send, o_recv, r_recv, t_send, t_recv, loc):
    s = lax.axis_index("seq")
    x = lax.axis_index("head")
    c = s % 2
    y = (s // 2) % NY
    z = s // (2 * NY)
    a = x * (1 - c) + y * c
    b = y * (1 - c) + x * c
    g = a + 4 * c
    r0 = y * 2 + c

    def dev(xx, yy, zz, cc):
        return ((zz * NY + yy) * 2 + cc, xx)

    def dev_ab(aa, bb, zz, cc):
        return dev(aa * (1 - c) + bb * c, bb * (1 - c) + aa * c, zz, cc)

    def remote(src, dst, send, recv, target):
        return pltpu.make_async_remote_copy(src_ref=src, dst_ref=dst, send_sem=send, recv_sem=recv,
                                            device_id=target, device_id_type=MESH)

    OFF = (0, U[0], U[0] + U[1])
    shared = U == FULL
    packs = (kpack, kpack if shared else vpack)
    total_u = sum(U)

    to_kin = pltpu.make_async_copy(k_ref, kin, loc.at[15])
    to_kin.start()

    row = lax.broadcasted_iota(jnp.int32, (4 * SEL, D), 0)
    lane = lax.broadcasted_iota(jnp.int32, (1, D), 1)
    names = jnp.full((4 * SEL, D), -1, jnp.int32)
    spots = jnp.zeros((1, D), jnp.int32)
    for h in range(NX):
        for e in range(SEL):
            block = sel_ref[h, e]
            name = jnp.where(e < count_ref[h], (block % NX) * (NZ * NY * 2) + block // NX, -1)
            names = jnp.where(row == h * SEL + e, name, names)
        spots = jnp.where(lane == h, own_ref[h], spots)
    key_ref[...] = names
    slot_ref[...] = spots

    barrier = pltpu.get_barrier_semaphore()

    def greet(target):
        pl.semaphore_signal(barrier, inc=1, device_id=target, device_id_type=MESH)

    greet(dev(x, y, z, 1 - c))
    for i in range(1, 4):
        for cc in range(2):
            greet(dev((x + i) % NX, y, z, cc))
            greet(dev(x, (y + i) % NY, z, cc))
    for i in range(1, NZ):
        greet(dev(x, y, (z + i) % NZ, c))
    pl.semaphore_wait(barrier, 20)

    def t_copy(n, receive):
        other = (r0 + n) % 8
        row = other if receive else r0
        target = dev(x, other // 2, z, other % 2)
        sem = (8 - n) % 8 if receive else n
        return (
            remote(key_ref, keyt.at[row], t_send.at[0, n], t_recv.at[0, sem], target),
            remote(slot_ref, slott.at[z, pl.ds(row, 1)], t_send.at[1, n], t_recv.at[1, sem], target),
        )

    def tz_copy(kind, n, receive):
        other = (z + n) % NZ
        row = other if receive else z
        sem = (8 - n) % 8 if receive else n
        buf = (slott, flags)[kind]
        return remote(buf.at[row], buf.at[row], t_send.at[2 + kind, n], t_recv.at[2 + kind, sem], dev(x, y, other, c))

    def t_local():
        return (pltpu.make_async_copy(key_ref, keyt.at[r0], loc.at[6]),
                pltpu.make_async_copy(slot_ref, slott.at[z, pl.ds(r0, 1)], loc.at[7]))

    kinds = ((kin, kn, D), (v_ref, vn, D), (q_ref, qbuf, GQ * D))

    def piece(kind, t, i):
        src, dst, width = kinds[kind]
        other = (x + i) % NX if t == 0 else (y + i) % NY
        head = other + 4 * t
        slot = (2 * x + c) if t == 0 else (2 * y + c)
        target = dev(other, y, z, 0) if t == 0 else dev(x, other, z, 1)
        src = src.at[:, pl.ds(pl.multiple_of(head * width, width), width)]
        return src, dst.at[slot], kind, t * 4 + i, slot, target

    def send_piece(kind, t, i):
        src, dst, kind, n, slot, target = piece(kind, t, i)
        remote(src, dst, ex_send.at[kind, n], ex_recv.at[kind, slot], target).start()

    def each_piece(kind, go_remote, go_local):
        for i in (2, 1, 3):
            for t in range(2):
                go_remote(kind, t, i)
        for t in range(2):
            @pl.when(c == t)
            def _():
                go_local(kind, t)

            @pl.when(c != t)
            def _():
                go_remote(kind, t, 0)

    def local_piece(kind, t):
        src, dst, _, _, _, _ = piece(kind, t, 0)
        return pltpu.make_async_copy(src, dst, loc.at[kind])

    def exchange(kind):
        each_piece(kind, send_piece, lambda kind, t: local_piece(kind, t).start())

    def wait_exchange(kind, places=(0, 1, 3, 2)):
        _, dst, _ = kinds[kind]

        def one(i, cc):
            aa = (a + i) % 4
            slot = 2 * aa + cc
            remote(dst.at[slot], dst.at[slot], ex_send.at[kind, 0], ex_recv.at[kind, slot], dev_ab(aa, b, z, cc)).wait_recv()

        for i in places:
            if i:
                for cc in range(2):
                    one(i, cc)
            else:
                one(0, 1 - c)
                for t in range(2):
                    @pl.when(c == t)
                    def _():
                        local_piece(kind, t).wait()

    def z_part(kind, way, hop, sub):
        bufs = ((kn, km, kf), (vn, vm, vf))[kind]
        at = ((0, 4, 3, 1, 0), (0, 1, 2, 0, 0))[way][hop] * GROUP + 2 * ((a + sub) % 4)
        return bufs[max(hop - 2, 0)].at[pl.ds(at, 2)]

    def z_copy(kind, way, step, sub):
        target = dev(x, y, (z + 1) % NZ if way == 0 else (z + 7) % NZ, c)
        return remote(z_part(kind, way, step - 1, sub), z_part(kind, way, step, sub),
                      z_send.at[kind, way, step - 1, sub], z_recv.at[kind, way, step - 1, sub], target)

    def z_parts(step):
        return [(way, sub) for sub in (0, 1, 3, 2) for way in range(2) if step < 4 or way == sub // 2]

    def z_first(kind):
        for sub in (0, 1, 3, 2):
            wait_exchange(kind, (sub,))
            for way in range(2):
                z_copy(kind, way, 1, sub).start()

    def z_hop(kind, step):
        for way, sub in z_parts(step):
            z_copy(kind, way, step, sub).wait_recv()
            if (way, sub) in z_parts(step + 1) and step < 4:
                z_copy(kind, way, step + 1, sub).start()

    up = dev_ab(a, (b + 1) % 4, z, c)
    down = dev_ab(a, (b + 3) % 4, z, c)

    def b_copy(kind, part, n):
        have = (ku, vu)[kind]
        rel = (krl, vrl)[kind]
        pack = packs[kind]
        u = U[part]
        h = u // 2
        p = 3 * OFF[part]
        f = HELD + p
        l = OFF[part]
        src, dst, target = (
            (pack.at[pl.ds(p, u)], have.at[pl.ds(f, u)], up),
            (pack.at[pl.ds(p + 2 * u, u)], have.at[pl.ds(f + 2 * u, u)], down),
            (pack.at[pl.ds(p + u, h)], rel.at[pl.ds(l, h)], up),
            (pack.at[pl.ds(p + u + h, h)], rel.at[pl.ds(l + h, h)], down),
            (rel.at[pl.ds(l, h)], have.at[pl.ds(f + u, h)], up),
            (rel.at[pl.ds(l + h, h)], have.at[pl.ds(f + u + h, h)], down),
        )[n]
        return remote(src, dst, b_send.at[kind, part, n], b_recv.at[kind, part, n], target)

    def b_begin(kind, part):
        bufs = ((kn, km, kf), (vn, vm, vf))[kind]
        pack = packs[kind]
        u = U[part]

        def one(r, _):
            for j in range(3):
                i = smem[2, (j + 1) * TW + OFF[part] + r]
                block = None
                for k in range(part + 1):
                    other = bufs[k][jnp.clip(i - STARTS[k], 0, CLASSES[k] - 1)]
                    block = other if k == 0 else lax.select(i >= STARTS[k], other, block)
                pack[3 * OFF[part] + j * u + r] = block
            return 0

        lax.fori_loop(0, u, one, 0)
        for n in (2, 3, 0, 1):
            b_copy(kind, part, n).start()

    def b_relay(kind, part):
        for n in (2, 3):
            b_copy(kind, part, n).wait_recv()
            b_copy(kind, part, n + 2).start()

    def b_end(kind, part):
        for n in (0, 1, 4, 5):
            b_copy(kind, part, n).wait_recv()

    def keep(kind, part):
        held = ((kn, km, kf), (vn, vm, vf))[kind][part]
        at = pl.ds(STARTS[part], CLASSES[part])
        return pltpu.make_async_copy(held, (ku, vu)[kind].at[at], loc.at[9 + 3 * kind + part])

    def keep_all(kind):
        for part in range(3):
            keep(kind, part).start()

    def kept(kind):
        for part in range(3):
            keep(kind, part).wait()

    def b_sent(kind):
        for part in range(3):
            for n in range(6):
                b_copy(kind, part, n).wait_send()

    def distance_class(t):
        off = (t // 32 - z + NZ) % NZ
        return jnp.where(off == 4, 2, jnp.where((off == 3) | (off == 5), 1, 0))

    def lists():
        f32, bf16, i32 = jnp.float32, jnp.bfloat16, jnp.int32
        n = NZ * NY * 2 * NX

        def one(hit):
            return jnp.where(hit, 1.0, 0.0).astype(f32)

        t_lane = lax.broadcasted_iota(i32, (NZ * NY * 2, n), 1)
        slots = slott[...].reshape(NZ * NY * 2, D)
        perm = jnp.concatenate([one(slots[:, h : h + 1] == t_lane) for h in range(NX)], axis=0).astype(bf16)
        keys = keyt[...].reshape(n, D)
        lane = lax.broadcasted_iota(i32, (n, D), 1)
        named = jnp.concatenate([one(keys == lane), one(keys == lane + D)], axis=1).astype(bf16)
        entry = jnp.dot(named, perm, preferred_element_type=f32)
        block = jnp.max(entry.reshape(4 * GROUP, SEL, n), axis=1)
        by_y = jnp.max(block.reshape(NY, GROUP, n), axis=1)
        by_x = functools.reduce(jnp.maximum, [block[i * NX : (i + 1) * NX] for i in range(2 * NY)])
        want = jnp.concatenate([by_y, by_x], axis=0)
        t0 = lax.broadcasted_iota(i32, (n, n), 0)
        t1 = lax.broadcasted_iota(i32, (n, n), 1)
        class0, class1 = distance_class(t0), distance_class(t1)
        before = (class0 < class1) | ((class0 == class1) & (t0 < t1))
        same_y = (t0 // 8) % NY == (t1 // 8) % NY
        same_x = t0 % NX == t1 % NX
        want_b = want.astype(bf16)

        def count(which):
            return jnp.dot(want_b, one(which).astype(bf16), preferred_element_type=f32)

        group = lax.broadcasted_iota(i32, (8, n), 0)
        t8 = lax.broadcasted_iota(i32, (8, n), 1)
        first = group < 4
        rank = jnp.where(first, count(before & same_y), count(before & same_x))
        n0, n1 = [jnp.where(first, count(same_y & (class0 == k)), count(same_x & (class0 == k))) for k in range(2)]
        away = jnp.where(first, (t8 // 8) % NY, t8 % NX) != group % 4
        class8 = distance_class(t8)
        rank = jnp.where(class8 >= 1, rank + jnp.maximum(U[0] - n0, 0.0), rank)
        rank = jnp.where(class8 == 2, rank + jnp.maximum(OFF[2] - n1 - jnp.maximum(n0, float(U[0])), 0.0), rank)
        over = one((want > 0.5) & away & (rank > total_u - 0.5))
        flags[z] = jnp.broadcast_to(jnp.max(over), (8, D)).astype(i32)
        wants[0] = want
        wants[1] = rank
        t = lax.broadcasted_iota(i32, (1, n), 1)
        tx, ty, tc, tz = t % NX, (t // 8) % NY, (t // 4) % 2, t // 32
        ta = tx * (1 - c) + ty * c
        tb = ty * (1 - c) + tx * c
        off = (tz - z + NZ) % NZ
        spot = jnp.where(off <= 2, off, jnp.where(off >= 6, off - 3, jnp.where(off == 4, 7, jnp.where(off == 3, 5, 6))))
        local = spot * GROUP + 2 * ta + tc

        def row(d):
            at = pl.ds(4 * c + d, 1)
            return wants[0, at, :], wants[1, at, :].astype(i32)

        _, rk = row(b)
        gap = (b - tb + 4) % 4 - 1
        shift = jnp.where(rk >= OFF[2], 2 * OFF[2] + gap * U[2], jnp.where(rk >= U[0], 2 * U[0] + gap * U[1], gap * U[0]))
        there = HELD + rk + shift
        at = jnp.clip(jnp.where(tb == b, local, there), 0, HELD + 3 * total_u - 1)
        r8 = lax.broadcasted_iota(i32, (8, n), 0)
        at8 = jnp.broadcast_to(at, (8, n))
        lhs = jnp.where(r8 == 0, at8 // 16, jnp.where(r8 == 1, at8 % 16, 1)).astype(f32).astype(bf16)
        got = lax.dot_general(lhs, entry.astype(bf16), (((1,), (1,)), ((), ())), preferred_element_type=f32)
        picks = []
        k = lax.broadcasted_iota(i32, (TW, n), 0)
        for j in range(4):
            wj, rj = row((b + j) % 4)
            kk = jnp.where((wj > 0.5) & (tb == b), rj, -1)
            picks.append(one(kk == k))
        picks = jnp.concatenate(picks, axis=0).astype(bf16)
        names = jnp.broadcast_to(local, (8, n)).astype(f32).astype(bf16)
        chosen = lax.dot_general(names, picks, (((1,), (1,)), ((), ())), preferred_element_type=f32)
        place = got[0:1] * 16.0 + got[1:2]
        index[0:1, :] = place.astype(i32)
        index[1:2, :] = got[2:3].astype(i32)
        index[2:3, :] = chosen[0:1].astype(i32)

    def to_scalars():
        return pltpu.make_async_copy(index, smem, loc.at[8])

    def entry_at(m):
        aa, cc = m // 2, m % 2
        yy = y * (1 - c) + aa * c
        xx = aa * (1 - c) + x * c
        return ((yy * 2 + cc) * NX + xx) * SEL

    def gather_entries(src, m):
        first = entry_at(m)
        for e in range(SEL):
            cat[e * ROWS : (e + 1) * ROWS, :] = src[jnp.clip(smem[0, first + e], 0, HELD + 3 * total_u - 1)]
        return first

    row = lax.broadcasted_iota(jnp.int32, (2 * ROWS, ROWS), 0) % ROWS
    col = lax.broadcasted_iota(jnp.int32, (2 * ROWS, ROWS), 1)
    seen = col <= row

    def scores(m, _):
        first = gather_entries(ku, m)
        bias = [jnp.where(smem[1, first + e] > 0, 0.0, -jnp.inf).astype(jnp.float32) for e in range(SEL)]

        def heads(h, _):
            two = qbuf[m, :, pl.ds(pl.multiple_of(h * 2 * D, 2 * D), 2 * D)]
            two = jnp.concatenate([two[:, :D], two[:, D:]], axis=0)
            sc = lax.dot_general(two, cat[...], (((1,), (1,)), ((), ())), preferred_element_type=jnp.float32)
            parts = [jnp.where(seen, sc[:, :ROWS], -jnp.inf)]
            parts += [sc[:, e * ROWS : (e + 1) * ROWS] + bias[e] for e in range(1, SEL)]
            top = functools.reduce(jnp.maximum, parts)
            top = jnp.max(top, axis=1, keepdims=True)
            parts = [jnp.exp2((p - top) * SCALE2) for p in parts]
            total = jnp.sum(functools.reduce(jnp.add, parts), axis=1, keepdims=True)
            inv = 1.0 / total
            at = pl.ds(pl.multiple_of(h * 2 * ROWS, 2 * ROWS), 2 * ROWS)
            for e in range(SEL):
                pbuf[m, at, e * ROWS : (e + 1) * ROWS] = (parts[e] * inv).astype(jnp.bfloat16)
            return 0

        lax.fori_loop(0, GQ // 2, heads, 0, unroll=2)
        return 0

    def columns(head):
        return out_ref.at[:, pl.ds(pl.multiple_of(head * GQ * D, GQ * D), GQ * D)]

    def out_copy(i, cc):
        m = 2 * ((a + i) % 4) + cc
        return remote(obuf.at[m], columns(g), o_send.at[2 * i + cc], o_recv.at[g], dev_ab((a + i) % 4, b, z, cc))

    def out_via(cc):
        m = 2 * ((a + 2) % 4) + cc
        step = 1 if cc == 0 else 3
        return remote(obuf.at[m], orl.at[cc], o_send.at[4 + cc], r_recv.at[cc], dev_ab((a + step) % 4, b, z, c))

    def out_relay(cc):
        step = 1 if cc == 0 else 3
        source = (a + 4 - step) % 4 + 4 * c
        return remote(orl.at[cc], columns(source), o_send.at[8 + cc], o_recv.at[source], dev_ab((a + step) % 4, b, z, cc))

    def out_local():
        return pltpu.make_async_copy(obuf.at[2 * a + c], columns(g), loc.at[5])

    def attend(n, _):
        q = n // 2
        i = jnp.where(q == 0, 2, jnp.where(q == 3, 0, 1 + 2 * (n % 2)))
        cc = jnp.where((q == 0) | (q == 3), n % 2, q - 1)
        m = 2 * ((a + i) % 4) + cc
        gather_entries(vu, m)

        def heads(h, _):
            at = pl.ds(pl.multiple_of(h * 2 * ROWS, 2 * ROWS), 2 * ROWS)
            o = jnp.dot(pbuf[m, at, :], cat[...], preferred_element_type=jnp.float32).astype(jnp.bfloat16)
            first = pl.multiple_of(h * 2 * D, 2 * D)
            obuf[m, :, pl.ds(first, D)] = o[:ROWS]
            obuf[m, :, pl.ds(pl.multiple_of(first + D, D), D)] = o[ROWS:]
            return 0

        lax.fori_loop(0, GQ // 2, heads, 0, unroll=2)
        for k in range(2):
            @pl.when(n == k)
            def _():
                out_via(k).start()
        for k in range(4):
            @pl.when(n == 2 + k)
            def _():
                out_copy(1 + 2 * (k % 2), k // 2).start()
        for k in range(2):
            @pl.when((n == 6 + k) & (c != k))
            def _():
                out_copy(0, k).start()

        @pl.when(n == 6 + c)
        def _():
            out_local().start()

        for k in range(2):
            @pl.when(n == 5 + k)
            def _():
                remote(orl.at[k], orl.at[k], o_send.at[4 + k], r_recv.at[k],
                       dev_ab((a + (3 if k == 0 else 1)) % 4, b, z, c)).wait_recv()
                out_relay(k).start()

        return 0

    to_kin.wait()
    exchange(0)
    for n in range(1, 8):
        for copy in t_copy(n, False):
            copy.start()
    for copy in t_local():
        copy.start()
    exchange(1)
    z_first(0)
    exchange(2)
    for n in range(1, 8):
        for copy in t_copy(n, True):
            copy.wait_recv()
    for copy in t_local():
        copy.wait()
    for n in range(1, 8):
        tz_copy(0, n, False).start()
    z_hop(0, 1)
    z_hop(0, 2)
    for n in range(1, 8):
        tz_copy(0, n, True).wait_recv()
    lists()
    to_scalars().start()
    for n in range(1, 8):
        tz_copy(1, n, False).start()
    to_scalars().wait()
    b_begin(0, 0)
    z_hop(0, 3)
    b_begin(0, 1)
    b_relay(0, 0)
    z_first(1)
    z_hop(0, 4)
    b_begin(0, 2)
    keep_all(0)
    b_relay(0, 1)
    z_hop(1, 1)
    b_relay(0, 2)
    z_hop(1, 2)
    if shared:
        b_sent(0)
    b_begin(1, 0)
    wait_exchange(2)
    b_end(0, 0)
    b_end(0, 1)
    kept(0)
    b_end(0, 2)
    lax.fori_loop(0, 2, scores, 0)
    z_hop(1, 3)
    b_begin(1, 1)
    b_relay(1, 0)
    lax.fori_loop(2, 4, scores, 0)
    z_hop(1, 4)
    b_begin(1, 2)
    keep_all(1)
    b_relay(1, 1)
    lax.fori_loop(4, 6, scores, 0)
    b_relay(1, 2)
    lax.fori_loop(6, 8, scores, 0)
    b_end(1, 0)
    b_end(1, 1)
    kept(1)
    b_end(1, 2)
    lax.fori_loop(0, 8, attend, 0)

    for n in range(1, 8):
        tz_copy(1, n, True).wait_recv()
    flag_ref[0, 0] = jnp.max(functools.reduce(jnp.maximum, [flags[i] for i in range(NZ)]))
    for n in range(1, 8):
        for copy in t_copy(n, False):
            copy.wait_send()
        for kind in range(2):
            tz_copy(kind, n, False).wait_send()
    for kind in range(3):
        def sent(kind, t, i):
            src, dst, kind, n, slot, target = piece(kind, t, i)
            remote(src, dst, ex_send.at[kind, n], ex_recv.at[kind, slot], target).wait_send()

        each_piece(kind, sent, lambda kind, t: None)
    for kind in range(2):
        for step in range(1, 5):
            for way, sub in z_parts(step):
                z_copy(kind, way, step, sub).wait_send()
    if not shared:
        b_sent(0)
    b_sent(1)
    for k in range(2):
        out_via(k).wait_send()
        out_relay(k).wait_send()
        for i in (1, 3):
            out_copy(i, k).wait_send()

        @pl.when(c != k)
        def _():
            out_copy(0, k).wait_send()
    out_local().wait()
    for h in range(8):
        dst = out_ref.at[:, pl.ds(h * GQ * D, GQ * D)]
        source = dev(h % 4, y, z, 0) if h < 4 else dev(x, h % 4, z, 1)

        @pl.when(g != h)
        def _():
            remote(dst, dst, o_send.at[0], o_recv.at[h], source).wait_recv()


def attention(U, ident, selected, counts, slots, queries, keys, values):
    any_space = pl.BlockSpec(memory_space=pl.ANY)
    smem = pl.BlockSpec(memory_space=pltpu.SMEM)
    block = (ROWS, D)
    bf16 = jnp.bfloat16
    dma = pltpu.SemaphoreType.DMA
    total = sum(U)
    return pl.pallas_call(
        functools.partial(kernel, U),
        out_shape=(pltpu.VMEM(queries.shape, bf16), jax.ShapeDtypeStruct((1, 1), jnp.int32)),
        in_specs=[smem] * 3 + [any_space] * 3,
        out_specs=(pl.BlockSpec(memory_space=pltpu.VMEM), smem),
        scratch_shapes=[
            pltpu.VMEM((4 * SEL, D), jnp.int32),
            pltpu.VMEM((1, D), jnp.int32),
            pltpu.VMEM(keys.shape, bf16),
            pltpu.VMEM((GROUP, ROWS, GQ * D), bf16),
            *[pltpu.VMEM((size, *block), bf16) for size in CLASSES * 2],
            pltpu.VMEM((HELD + 3 * total, *block), bf16),
            pltpu.VMEM((HELD + 3 * total, *block), bf16),
            pltpu.VMEM((3 * total, *block), bf16),
            pltpu.VMEM((1 if U == FULL else 3 * total, *block), bf16),
            pltpu.VMEM((total, *block), bf16),
            pltpu.VMEM((total, *block), bf16),
            pltpu.VMEM((SEL * ROWS, D), bf16),
            pltpu.VMEM((GROUP, GQ * ROWS, SEL * ROWS), bf16),
            pltpu.VMEM((GROUP, ROWS, GQ * D), bf16),
            pltpu.VMEM((2, ROWS, GQ * D), bf16),
            pltpu.VMEM((8, 4 * SEL, D), jnp.int32),
            pltpu.VMEM((NZ, 8, D), jnp.int32),
            pltpu.VMEM((2, 8, 256), jnp.float32),
            pltpu.VMEM((8, 256), jnp.int32),
            pltpu.SMEM((8, 256), jnp.int32),
            pltpu.VMEM((NZ, 8, D), jnp.int32),
            dma((3, 8)), dma((3, 8)),
            dma((2, 2, 4, 4)), dma((2, 2, 4, 4)),
            dma((2, 3, 6)), dma((2, 3, 6)),
            dma((10,)), dma((8,)), dma((2,)),
            dma((4, 8)), dma((4, 8)),
            dma((16,)),
        ],
        compiler_params=pltpu.CompilerParams(
            collective_id=ident, has_side_effects=True, vmem_limit_bytes=(58 if U == FULL else 44) * 1024 * 1024),
    )(selected, counts, slots, queries, keys, values)


def body(queries, keys, values, selected, counts, block_slot):
    tables = (selected, counts, block_slot)
    out, flag = attention(FAST, 0, *tables, queries, keys, values)
    again = lambda: attention(FULL, 1, *tables, queries, keys, values)[0]
    return lax.cond(flag[0, 0] > 0, again, lambda: out)


def solution(mesh):
    return jax.shard_map(
        body,
        mesh=mesh,
        in_specs=(
            P(("seq", "head"), None),
            P(("seq", "head"), None),
            P(("seq", "head"), None),
            P("seq", None),
            P("seq"),
            P("seq"),
        ),
        out_specs=P(("seq", "head"), None),
        check_vma=False,
    )
```
